256 devices in a mesh: band: 4 (over x), blk: 64 (over z, y, core).
Axes of the slice: x: 4, y: 4, z: 8, core: 2. Of those that a mesh axis runs over, the one named last changes fastest.
Arguments:
- solution: float32 [9, 2, 2048, 2048], P(None, None, 'blk', 'band'), may hold values from -6 to 6
- residual: float32 [9, 2, 2048, 2048], P(None, None, 'blk', 'band'), may hold values from -20 to 20
- direction: float32 [9, 2, 2048, 2048], P(None, None, 'blk', 'band'), may hold values from -20 to 20
- precond: float32 [9, 2048], P(None, 'band'), may hold values from 0.2 to 2
- inv_spec: float32 [9, 2048], P(None, 'band'), may hold values from 0.05 to 2
- mixing: float32 [9, 3], replicated, may hold values from 0.1 to 2.5
- beams: float32 [9, 2048], replicated, may hold values from 0.2 to 1
- slot_band: int32 [12], replicated, may hold values from 0 to 11, each once
- m_order: int32 [2048], replicated, may hold values from 0 to 2047, each once
- cycle_order: int32 [1024], replicated, may hold values from 0 to 1023, each once
- inv_noise: float32 [12, 3, 1024, 4096], P('band', None, 'blk'), may hold values from 0.3 to 3
- pix_mask: int32 [1024, 4096], P('blk'), may hold values 0 or 1
Outputs:
- solution_next: float32 [9, 2, 2048, 2048], P(None, None, 'blk', 'band')
- residual_next: float32 [9, 2, 2048, 2048], P(None, None, 'blk', 'band')
- direction_next: float32 [9, 2, 2048, 2048], P(None, None, 'blk', 'band')
The draws below stay inside these ranges and needn't reach their ends.
Inputs may be any that keep to these rules, and one draw needn't show every extreme that they name: `slot_band`: slots holding a value of 9 or more are empty; each band lies in exactly one slot. `m_order`: each order 0 to 2047 appears once. `cycle_order`: each cycle 0 to 1023 appears once.
All inputs are finite; a program needn't handle non-finite values. No bound on the sum of `pix_mask` on one device may be relied on, other than what follows from the above.
Results may differ from the reference program's by a relative error of at most 0.0075.
Values may be sent and summed in bfloat16 or wider, within the bound.
A program may use at most 128 MiB of HBM per device.

```python
import math
import jax
import jax.numpy as jnp
from jax import lax

COMP = 3
STOKES = 3
FIELDS = 9
BANDS = 9
SLOTS_ALL = 12
L = 2048
M_DEV = 32
MODES = 2048
CYCLES = 1024
PHI = 4096


def rising_field(key, salt):
    folded = jax.random.fold_in(key, salt)
    base = jax.random.truncated_normal(folded, -4.0, 4.0, (FIELDS, 2, MODES, L), jnp.float32)
    m_rise = 0.5 + jnp.arange(MODES, dtype=jnp.float32) / MODES
    l_rise = 0.5 + jnp.arange(L, dtype=jnp.float32) / L
    block_total = MODES // M_DEV
    block_key = jax.random.fold_in(folded, 3)
    block_scale = jnp.exp(jax.random.uniform(block_key, (block_total,), jnp.float32, math.log(0.4), math.log(2.5)))
    scaling = m_rise[:, None] * l_rise[None, :]
    row_scale = jnp.repeat(block_scale, M_DEV)
    scaling = scaling * row_scale[:, None]
    return jnp.clip(base * scaling, -20.0, 20.0)


def draw_residual(key, part):
    return rising_field(key, 11)


def draw_direction(key, part):
    return rising_field(key, 23)


def touch_ends(entries, key, least, high):
    place = [jax.random.randint(jax.random.fold_in(key, axis), (), 0, length) for axis, length in enumerate(entries.shape)]
    main_axis = entries.shape.index(max(entries.shape))
    next_to = place[:main_axis] + [(place[main_axis] + 1) % entries.shape[main_axis]] + place[main_axis + 1:]
    return entries.at[tuple(place)].set(least).at[tuple(next_to)].set(high)


def block_levels(stream_key, shape, cuts, low, largest):
    def one(axis_at, parts):
        steps = jax.random.uniform(jax.random.fold_in(jax.random.fold_in(stream_key, 6), axis_at), (parts,), jnp.float32, low / len(cuts), largest / len(cuts))
        return jnp.repeat(jnp.exp(steps), shape[axis_at] // parts).reshape((-1,) + (1,) * (len(shape) - axis_at - 1))

    level = one(*cuts[0])
    for cut in cuts[1:]:
        level = level * one(*cut)
    return level


def gaussian(own_key, shape, deviation, limit, split=(), held_as=jnp.bfloat16):
    gain = block_levels(own_key, shape, split, -0.22, 0.18) if split else 1.0
    drawn = jax.random.normal(own_key, shape, jnp.float32) * deviation * gain
    return jnp.minimum(jnp.maximum(drawn, -limit), limit).astype(held_as)


def setup_inputs(seed: int = 0) -> dict:
    key_list = jax.random.split(jax.random.key(seed), 13)
    return {
        "solution": gaussian(key_list[0], (FIELDS, 2, MODES, L), 1.0, 6.0, ((2, 64), (3, 4)), jnp.float32),
        "residual": draw_residual(jax.random.fold_in(key_list[12], 71), 0),
        "direction": draw_direction(jax.random.fold_in(key_list[12], 71), 0),
        "precond": jnp.clip(jnp.exp(math.log(2.0) - 2.3025851 * jax.random.uniform(key_list[3], (FIELDS, L), jnp.float32) ** block_levels(key_list[3], (FIELDS, L), ((1, 4),), -0.2, 0.2)), 0.2, 2.0),
        "inv_spec": jnp.clip(jnp.exp(math.log(2.0) - 3.6888794 * jax.random.uniform(key_list[4], (FIELDS, L), jnp.float32) ** block_levels(key_list[4], (FIELDS, L), ((1, 4),), -0.2, 0.2)), 0.05, 2.0),
        "mixing": jnp.clip(jnp.exp(jax.random.uniform(key_list[5], (BANDS, COMP), jnp.float32, math.log(0.1), math.log(2.5))), 0.1, 2.5),
        "beams": jnp.clip(jnp.exp(jax.random.uniform(key_list[6], (BANDS, L), jnp.float32, math.log(0.2), math.log(1.0))), 0.2, 1.0),
        "slot_band": jax.random.permutation(key_list[7], SLOTS_ALL).astype(jnp.int32),
        "m_order": jax.random.permutation(key_list[8], MODES).astype(jnp.int32),
        "cycle_order": jax.random.permutation(key_list[9], CYCLES).astype(jnp.int32),
        "inv_noise": jnp.clip(jnp.exp(math.log(3.0) - 2.3025851 * jax.random.uniform(key_list[10], (SLOTS_ALL, STOKES, CYCLES, PHI), jnp.float32) ** block_levels(key_list[10], (SLOTS_ALL, STOKES, CYCLES, PHI), ((0, 4), (2, 64)), -0.2, 0.2)), 0.3, 3.0),
        "pix_mask": touch_ends((jax.random.randint(key_list[11], (CYCLES, PHI), 0, 4) < 3).astype(jnp.int32), jax.random.fold_in(key_list[11], 1), 0, 1),
    }


def rounded(values):
    return lax.optimization_barrier(values.astype(jnp.bfloat16)).astype(jnp.float32)

def legendre_table(cycle_order, l_total, cycle_total):
    l_values = jnp.arange(l_total, dtype=jnp.int32)
    phase_int = l_values[None, :] * (2 * cycle_order[:, None] + 1) % (4 * cycle_total)
    angles = phase_int.astype(jnp.float32) * (math.pi / (2 * cycle_total))
    return (jnp.cos(angles) / math.sqrt(l_total)).astype(jnp.bfloat16)

def fourier_block(m_order, first_cell, block_width, phi_total):
    phi_cells = first_cell + jnp.arange(block_width, dtype=jnp.int32)
    phase_int = m_order[:, None] * phi_cells[None, :] % phi_total
    angles = phase_int.astype(jnp.float32) * (2.0 * math.pi / phi_total)
    scaling = 1.0 / math.sqrt(m_order.shape[0])
    return jnp.stack([jnp.cos(angles) * scaling, -jnp.sin(angles) * scaling]).astype(jnp.bfloat16)

def reference(solution, residual, direction, precond, inv_spec, mixing, beams, slot_band, m_order, cycle_order, inv_noise, pix_mask):
    highest = lax.Precision.HIGHEST
    colat = legendre_table(cycle_order, L, CYCLES).astype(jnp.float32)
    azim = fourier_block(m_order, 0, PHI, PHI).astype(jnp.float32)
    triangle = (jnp.arange(L, dtype=jnp.int32)[None, :] >= m_order[:, None]).astype(jnp.float32)
    select = (slot_band[:, None] == jnp.arange(BANDS, dtype=jnp.int32)[None, :]).astype(jnp.float32)
    slot_mix = jnp.dot(select, mixing, precision=highest)
    slot_beam = jnp.dot(select, beams, precision=highest)
    halved = direction.astype(jnp.bfloat16).astype(jnp.float32).reshape(COMP, STOKES, 2, MODES, L)
    weight = inv_noise * pix_mask.astype(jnp.float32)[None, None]

    def one_slot(running, slot_index):
        mix_row = slot_mix[slot_index]
        beam_row = slot_beam[slot_index]
        mixed_sum = lax.optimization_barrier(jnp.sum(mix_row[:, None, None, None, None] * halved, axis=0))
        amplitudes = rounded(mixed_sum * beam_row[None, None, None, :] * triangle[None, None])
        colat_side = rounded(jnp.einsum('xkml,rl->xkmr', amplitudes, colat, precision=highest))
        sky_part = jnp.einsum('xkmr,kmp->xrp', colat_side, azim, precision=highest)
        weighted = rounded(weight[slot_index] * sky_part)
        back_cycle = rounded(jnp.einsum('xrp,kmp->xkmr', weighted, azim, precision=highest))
        back_harm = jnp.einsum('xkmr,rl->xkml', back_cycle, colat, precision=highest)
        back_harm = back_harm * beam_row[None, None, None, :] * triangle[None, None]
        term = mix_row[:, None, None, None, None] * back_harm[None]
        return (running + term.reshape(FIELDS, 2, MODES, L), None)
    zero_carry = jnp.zeros((FIELDS, 2, MODES, L), jnp.float32)
    band_term, _ = lax.scan(one_slot, zero_carry, jnp.arange(SLOTS_ALL, dtype=jnp.int32))
    prior_diag = inv_spec[:, None, None, :]
    precond_full = precond[:, None, None, :]
    applied = prior_diag * direction + band_term
    scaled_res = precond_full * residual
    norm_old = jnp.sum(residual * scaled_res)
    curvature = jnp.sum(direction * applied)
    step_size = norm_old / curvature
    solution_next = solution + step_size * direction
    residual_next = residual - step_size * applied
    scaled_next = precond_full * residual_next
    norm_new = jnp.sum(residual_next * scaled_next)
    direction_next = scaled_next + norm_new / norm_old * direction
    return (solution_next, residual_next, direction_next)
```

```python
import functools
import math

import jax
import jax.numpy as jnp
from jax import lax
from jax.experimental import pallas as pl
from jax.experimental.pallas import tpu as pltpu
from jax.sharding import Mesh
from jax.sharding import PartitionSpec as P

COMP = 3
STOKES = 3
FIELDS = 9
BANDS = 9
SLOTS = 3
PAIRS = SLOTS * STOKES
L = 2048
CYCLES = 1024
MODES = 2048
PHI = 4096
QUARTER = PHI // 4
M_DEV = 32
R_DEV = 16
BLOCKS = 64
L_DEV = 512
LANES = PAIRS * 2 * M_DEV
BLK = ("blk_0", "blk_1", "blk_2")
BAND_BLK = ("band", "blk_0", "blk_1", "blk_2")
SCALE = 1.0 / math.sqrt(2048)
VMEM = pltpu.VMEM
F32 = jnp.float32
BF16 = jnp.bfloat16
NT = (((1,), (1,)), ((), ()))
NN = (((1,), (0,)), ((), ()))


def in_vmem():
    return pl.BlockSpec(memory_space=VMEM)


def in_smem():
    return pl.BlockSpec(memory_space=pltpu.SMEM)


def unit_circle(turn):
    half = (((turn + 2048) & 4095) - 2048).astype(F32) * (math.pi / 4096)
    sq = half * half
    sine = half * (
        1
        + sq
        * (-1 / 6 + sq * (1 / 120 + sq * (-1 / 5040 + sq * (1 / 362880 + sq * (-1 / 39916800)))))
    )
    cosine = 1 + sq * (
        -1 / 2
        + sq
        * (
            1 / 24
            + sq * (-1 / 720 + sq * (1 / 40320 + sq * (-1 / 3628800 + sq * (1 / 479001600))))
        )
    )
    return cosine * cosine - sine * sine, 2 * sine * cosine


def first_turns(mult):
    lane = lax.broadcasted_iota(jnp.int32, mult.shape, 1)
    cosine, sine = unit_circle((mult * lane) & 4095)
    step_cos, step_sin = unit_circle((mult * 128) & 4095)
    return cosine * SCALE, sine * SCALE, step_cos, step_sin


def colat_rows(mult, store):
    cosine, sine, step_cos, step_sin = first_turns(mult)
    for tile in range(L // 128):
        store(tile, cosine.astype(BF16))
        cosine, sine = cosine * step_cos - sine * step_sin, sine * step_cos + cosine * step_sin


def azim_rows(mult, store):
    cosine, sine, step_cos, step_sin = first_turns(mult)
    for tile in range(QUARTER // 128):
        store(tile, cosine.astype(BF16), (-sine).astype(BF16))
        cosine, sine = cosine * step_cos - sine * step_sin, sine * step_cos + cosine * step_sin


def tables_kernel(cycle_mult, order_mult, colat, azim):
    @pl.loop(0, cycle_mult.shape[0] // 32)
    def _(block):
        rows = pl.ds(pl.multiple_of(block * 32, 32), 32)

        def put(tile, value):
            colat[rows, tile * 128 : (tile + 1) * 128] = value

        colat_rows(cycle_mult[rows, :], put)

    @pl.loop(0, order_mult.shape[0] // 32)
    def _(block):
        rows = pl.ds(pl.multiple_of(block * 32, 32), 32)
        real_rows = pl.ds(pl.multiple_of(block * 64, 32), 32)
        imag_rows = pl.ds(pl.multiple_of(block * 64 + 32, 32), 32)

        def put(tile, real, imag):
            azim[real_rows, tile * 128 : (tile + 1) * 128] = real
            azim[imag_rows, tile * 128 : (tile + 1) * 128] = imag

        azim_rows(order_mult[rows, :], put)


def make_tables(cycle_mult, order_mult):
    steps = 8
    return pl.pallas_call(
        tables_kernel,
        grid=(steps,),
        in_specs=[
            pl.BlockSpec((CYCLES // steps, 128), lambda g: (g, 0)),
            pl.BlockSpec((MODES // steps, 128), lambda g: (g, 0)),
        ],
        out_specs=[
            pl.BlockSpec((CYCLES // steps, L), lambda g: (g, 0)),
            pl.BlockSpec((2 * MODES // steps, QUARTER), lambda g: (g, 0)),
        ],
        out_shape=[
            jax.ShapeDtypeStruct((CYCLES, L), BF16),
            jax.ShapeDtypeStruct((2 * MODES, QUARTER), BF16),
        ],
        cost_estimate=pl.CostEstimate(
            flops=60_000_000, bytes_accessed=14_000_000, transcendentals=0
        ),
        name="tables",
    )(cycle_mult, order_mult)


def at_least(orders, first, width):
    l_values = first + lax.broadcasted_iota(jnp.int32, (M_DEV, width), 1)
    return (l_values >= orders).astype(F32)


def forward_kernel(pieces, colat, beam, orders, mix, out, amps):
    for piece in range(4):
        for half in range(2):
            first = piece * L_DEV + half * 256
            cols = slice(half * 256, half * 256 + 256)
            triangle = at_least(orders[:, 0:1], first, 256)
            for s in range(STOKES):
                for k in range(2):
                    comps = [
                        pieces[piece, c * 3 + s, k, :, cols].astype(F32) for c in range(COMP)
                    ]
                    for x in range(SLOTS):
                        mixed = mix[x, 0] * comps[0]
                        for c in range(1, COMP):
                            mixed = mixed + mix[x, c] * comps[c]
                        row = ((s * 3 + x) * 2 + k) * M_DEV
                        value = mixed * beam[x : x + 1, first : first + 256] * triangle
                        amps[row : row + M_DEV, first : first + 256] = value.astype(BF16)

    @pl.loop(0, CYCLES // 256)
    def _(block):
        rows = pl.ds(pl.multiple_of(block * 256, 256), 256)
        out[rows, :] = lax.dot_general(
            colat[rows, :], amps[...], NT, preferred_element_type=F32
        ).astype(BF16)


def forward(pieces, colat, beam, orders, mix):
    return pl.pallas_call(
        forward_kernel,
        in_specs=[in_vmem(), in_vmem(), in_vmem(), in_vmem(), in_smem()],
        out_specs=in_vmem(),
        out_shape=jax.ShapeDtypeStruct((CYCLES, LANES), BF16),
        scratch_shapes=[VMEM((LANES, L), BF16)],
        cost_estimate=pl.CostEstimate(
            flops=2 * CYCLES * L * LANES, bytes_accessed=8_000_000, transcendentals=0
        ),
        name="forward",
    )(pieces, colat, beam, orders, mix)


def partner(value, low):
    return jnp.where(low, pltpu.roll(value, 96, 1), pltpu.roll(value, 32, 1))


def sky_kernel(arrived, azim, noise, mask, turns, out, turned, weighted):
    lane = lax.broadcasted_iota(jnp.int32, (R_DEV, 128), 1)
    left = lane < 64
    low = (lane & 63) < 32

    @pl.loop(0, BLOCKS // 2)
    def _(tile):
        cols = pl.ds(pl.multiple_of(tile * 128, 128), 128)
        sign, cosine, sine = turns[0:1, cols], turns[1:2, cols], turns[2:3, cols]
        for column in range((PAIRS + 1) // 2):
            end = min(column * 128 + 128, LANES)
            first = arrived[2 * tile, :, column * 128 : end].astype(F32)
            second = arrived[2 * tile + 1, :, column * 128 : end].astype(F32)
            if end - column * 128 == 64:
                values = [jnp.concatenate([first, second], axis=1)]
            else:
                values = [
                    jnp.where(left, first, pltpu.roll(second, 64, 1)),
                    jnp.where(left, pltpu.roll(first, 64, 1), second),
                ]
            for offset, value in enumerate(values):
                s, x = divmod(column * 2 + offset, 3)
                straight = cosine * value
                crossed = sine * partner(value, low)
                for q, part in enumerate(
                    (value, straight - crossed, sign * value, straight + crossed)
                ):
                    row = s * 192 + q * 48 + x * R_DEV
                    turned[row : row + R_DEV, cols] = part.astype(BF16)

    @pl.loop(0, QUARTER // 256)
    def _(block):
        start = pl.multiple_of(block * 256, 256)
        cols = pl.ds(start, 256)
        sky = lax.dot_general(turned[...], azim[:, cols], NN, preferred_element_type=F32)
        for q in range(4):
            cells = pl.ds(pl.multiple_of(q * QUARTER + start, 256), 256)
            keep = mask[:, cells].astype(F32)
            for s in range(STOKES):
                for x in range(SLOTS):
                    row = s * 192 + q * 48 + x * R_DEV
                    weight = noise[x, s, :, cells] * keep
                    weighted[row : row + R_DEV, cols] = (
                        weight * sky[row : row + R_DEV, :]
                    ).astype(BF16)

    @pl.loop(0, BLOCKS // 4)
    def _(block):
        rows = pl.ds(pl.multiple_of(block * 256, 256), 256)
        back = lax.dot_general(weighted[...], azim[rows, :], NT, preferred_element_type=F32)
        for sub in range(2):
            tile = block * 2 + sub
            cols = pl.ds(pl.multiple_of(tile * 128, 128), 128)
            sign, cosine, sine = turns[0:1, cols], turns[1:2, cols], turns[2:3, cols]
            lanes = slice(sub * 128, sub * 128 + 128)
            values = []
            for s in range(STOKES):
                for x in range(SLOTS):
                    base = s * 192 + x * R_DEV
                    b0, b1, b2, b3 = (
                        back[base + q * 48 : base + q * 48 + R_DEV, lanes] for q in range(4)
                    )
                    values.append(
                        b0 + sign * b2 + cosine * (b1 + b3) + sine * partner(b1 - b3, low)
                    )
            for column in range(PAIRS // 2):
                even, odd = values[2 * column], values[2 * column + 1]
                span = slice(column * 128, column * 128 + 128)
                out[2 * tile, :, span] = jnp.where(left, even, pltpu.roll(odd, 64, 1)).astype(BF16)
                out[2 * tile + 1, :, span] = jnp.where(left, pltpu.roll(even, 64, 1), odd).astype(
                    BF16
                )
            last = values[-1]
            out[2 * tile, :, LANES - 64 :] = last[:, :64].astype(BF16)
            out[2 * tile + 1, :, LANES - 64 :] = last[:, 64:].astype(BF16)


def sky_pass(arrived, azim, noise, mask, turns):
    return pl.pallas_call(
        sky_kernel,
        in_specs=[in_vmem()] * 5,
        out_specs=in_vmem(),
        out_shape=jax.ShapeDtypeStruct((BLOCKS, R_DEV, LANES), BF16),
        scratch_shapes=[VMEM((4 * PAIRS * R_DEV, 4096), BF16), VMEM((4 * PAIRS * R_DEV, QUARTER), BF16)],
        cost_estimate=pl.CostEstimate(
            flops=2 * 2 * 576 * 4096 * 1024, bytes_accessed=14_000_000, transcendentals=0
        ),
        name="sky",
    )(arrived, azim, noise, mask, turns)


def back_kernel(returned, colat, beam, orders, mix, out, flipped):
    for column in range(LANES // 64):
        lanes = slice(column * 64, column * 64 + 64)
        flipped[lanes, :] = returned[:, lanes].astype(F32).T.astype(BF16)

    @pl.loop(0, L // 256)
    def _(block):
        start = pl.multiple_of(block * 256, 256)
        cols = pl.ds(start, 256)
        harm = lax.dot_general(flipped[...], colat[:, cols], NN, preferred_element_type=F32)
        triangle = at_least(orders[:, 0:1], start, 256)
        piece = block // 2
        inner = pl.ds(pl.multiple_of((block % 2) * 256, 256), 256)
        for s in range(STOKES):
            for k in range(2):
                shaped = []
                for x in range(SLOTS):
                    row = ((s * 3 + x) * 2 + k) * M_DEV
                    shaped.append(harm[row : row + M_DEV, :] * beam[x : x + 1, cols] * triangle)
                for c in range(COMP):
                    total = mix[0, c] * shaped[0]
                    for x in range(1, SLOTS):
                        total = total + mix[x, c] * shaped[x]
                    out[piece, c * 3 + s, k, :, inner] = total.astype(BF16)


def back(returned, colat, beam, orders, mix):
    return pl.pallas_call(
        back_kernel,
        in_specs=[in_vmem(), in_vmem(), in_vmem(), in_vmem(), in_smem()],
        out_specs=in_vmem(),
        out_shape=jax.ShapeDtypeStruct((4, FIELDS, 2, M_DEV, L_DEV), BF16),
        scratch_shapes=[VMEM((LANES, CYCLES), BF16)],
        cost_estimate=pl.CostEstimate(
            flops=2 * CYCLES * L * LANES, bytes_accessed=8_000_000, transcendentals=0
        ),
        name="back",
    )(returned, colat, beam, orders, mix)


def slot_tables(my_slots, mixing, beams):
    select = (my_slots[:, None] == jnp.arange(BANDS, dtype=jnp.int32)[None, :]).astype(F32)
    highest = lax.Precision.HIGHEST
    return (jnp.dot(select, mixing, precision=highest), jnp.dot(select, beams, precision=highest))


def quarter_turns(m_order):
    m_lane = jnp.broadcast_to(m_order.reshape(BLOCKS, 1, M_DEV), (BLOCKS, 2, M_DEV))
    part = jnp.array([1.0, -1.0], F32)[None, :, None]
    phase = m_lane % 4
    sign = jnp.where(phase % 2 == 0, 1.0, -1.0).astype(F32)
    cosine = jnp.where(phase == 0, 1.0, jnp.where(phase == 2, -1.0, 0.0)).astype(F32)
    sine = jnp.where(phase == 1, 1.0, jnp.where(phase == 3, -1.0, 0.0)).astype(F32) * part
    rows = jnp.stack([sign, cosine, sine]).reshape(3, 2 * MODES)
    return jnp.concatenate([rows, jnp.zeros((5, 2 * MODES), F32)])


def on_device(
    solution,
    residual,
    direction,
    precond,
    inv_spec,
    mixing,
    beams,
    slot_band,
    m_order,
    cycle_order,
    inv_noise,
    pix_mask,
):
    band_index = lax.axis_index("band")
    block_index = lax.axis_index(BLK)
    halved = direction.astype(BF16)
    pieces = lax.all_to_all(
        jnp.broadcast_to(halved[None], (4, *halved.shape)), "band", 0, 0, tiled=True
    )
    cycle_mult = jnp.broadcast_to((2 * cycle_order + 1)[:, None], (CYCLES, 128))
    order_mult = jnp.broadcast_to(m_order[:, None], (MODES, 128))
    colat, azim = make_tables(cycle_mult, order_mult)
    turns = quarter_turns(m_order)
    my_orders = lax.dynamic_slice_in_dim(m_order, block_index * M_DEV, M_DEV)
    orders = jnp.broadcast_to(my_orders[:, None], (M_DEV, 128))
    my_slots = lax.dynamic_slice_in_dim(slot_band, band_index * SLOTS, SLOTS)
    slot_mix, slot_beam = slot_tables(my_slots, mixing, beams)
    colat_side = forward(pieces, colat, slot_beam, orders, slot_mix)
    cycle_side = lax.all_to_all(
        colat_side.reshape(BLOCKS, R_DEV, LANES), BLK, split_axis=0, concat_axis=0, tiled=True
    )
    weighted_back = sky_pass(cycle_side, azim, inv_noise, pix_mask, turns)
    returned = lax.all_to_all(weighted_back, BLK, split_axis=0, concat_axis=0, tiled=True)
    combined = back(returned.reshape(CYCLES, LANES), colat, slot_beam, orders, slot_mix)
    parts = lax.all_to_all(combined, "band", 0, 0, tiled=True)
    data_term = jnp.sum(parts.astype(F32), axis=0)
    prior_diag = inv_spec[:, None, None, :]
    precond_full = precond[:, None, None, :]
    applied = prior_diag * direction + data_term
    scaled_res = precond_full * residual
    sums = jnp.stack(
        [
            jnp.sum(residual * scaled_res),
            jnp.sum(direction * applied),
            jnp.sum(applied * scaled_res),
            jnp.sum(applied * precond_full * applied),
        ]
    )
    norm_old, curvature, crossed, squared = lax.psum(sums, BAND_BLK)
    step_size = norm_old / curvature
    solution_next = solution + step_size * direction
    residual_next = residual - step_size * applied
    scaled_next = precond_full * residual_next
    norm_new = norm_old - 2.0 * step_size * crossed + step_size * step_size * squared
    direction_next = scaled_next + norm_new / norm_old * direction
    return (solution_next, residual_next, direction_next)


def solution(mesh):
    finer = Mesh(
        mesh.devices.reshape(mesh.shape["band"], 8, 4, 2), ("band", "blk_0", "blk_1", "blk_2")
    )
    in_specs = (
        P(None, None, BLK, "band"),
        P(None, None, BLK, "band"),
        P(None, None, BLK, "band"),
        P(None, "band"),
        P(None, "band"),
        P(),
        P(),
        P(),
        P(),
        P(),
        P("band", None, BLK, None),
        P(BLK, None),
    )
    out_specs = (P(None, None, BLK, "band"), P(None, None, BLK, "band"), P(None, None, BLK, "band"))
    return jax.shard_map(
        on_device, mesh=finer, in_specs=in_specs, out_specs=out_specs, check_vma=False
    )
```

```python
import math

import jax
import jax.numpy as jnp
from jax import lax
from jax.experimental import pallas as pl
from jax.experimental.pallas import tpu as pltpu
from jax.sharding import Mesh
from jax.sharding import PartitionSpec as P

COMP = 3
STOKES = 3
FIELDS = 9
BANDS = 9
SLOTS = 3
L = 2048
CYCLES = 1024
MODES = 2048
PHI = 4096
QUARTER = PHI // 4
M_DEV = 32
R_DEV = 16
BLOCKS = 64
L_DEV = 512
BLK = ("blk_0", "blk_1", "blk_2")
SCALE = 1.0 / math.sqrt(2048)
VMEM = pltpu.VMEM
MESH = pl.DeviceIdType.MESH
F32 = jnp.float32
BF16 = jnp.bfloat16
NT = (((1,), (1,)), ((), ()))
NN = (((1,), (0,)), ((), ()))


def in_vmem():
    return pl.BlockSpec(memory_space=VMEM)


def in_smem():
    return pl.BlockSpec(memory_space=pltpu.SMEM)


def unit_circle(turn):
    half = (((turn + 2048) & 4095) - 2048).astype(F32) * (math.pi / 4096)
    sq = half * half
    sine = half * (
        1
        + sq
        * (-1 / 6 + sq * (1 / 120 + sq * (-1 / 5040 + sq * (1 / 362880 + sq * (-1 / 39916800)))))
    )
    cosine = 1 + sq * (
        -1 / 2
        + sq
        * (
            1 / 24
            + sq * (-1 / 720 + sq * (1 / 40320 + sq * (-1 / 3628800 + sq * (1 / 479001600))))
        )
    )
    return cosine * cosine - sine * sine, 2 * sine * cosine


def first_turns(mult):
    lane = lax.broadcasted_iota(jnp.int32, mult.shape, 1)
    cosine, sine = unit_circle((mult * lane) & 4095)
    step_cos, step_sin = unit_circle((mult * 128) & 4095)
    return cosine * SCALE, sine * SCALE, step_cos, step_sin


def colat_rows(mult, store):
    cosine, sine, step_cos, step_sin = first_turns(mult)
    for tile in range(L // 128):
        store(tile, cosine.astype(BF16))
        cosine, sine = cosine * step_cos - sine * step_sin, sine * step_cos + cosine * step_sin


def azim_rows(mult, store):
    cosine, sine, step_cos, step_sin = first_turns(mult)
    for tile in range(QUARTER // 128):
        store(tile, cosine.astype(BF16), (-sine).astype(BF16))
        cosine, sine = cosine * step_cos - sine * step_sin, sine * step_cos + cosine * step_sin


def at_least(orders, first, width):
    l_values = first + lax.broadcasted_iota(jnp.int32, (M_DEV, width), 1)
    return (l_values >= orders).astype(F32)


def partner(value, low):
    return jnp.where(low, pltpu.roll(value, 96, 1), pltpu.roll(value, 32, 1))


def folded(value):
    tiles = [
        value[8 * i : 8 * i + 8, 128 * j : 128 * j + 128]
        for i in range(value.shape[0] // 8)
        for j in range(value.shape[1] // 128)
    ]
    while len(tiles) > 1:
        tiles = [first + second for first, second in zip(tiles[::2], tiles[1::2])]
    return tiles[0]


def operator_kernel(
    direction_in,
    residual_in,
    noise_in,
    mask_in,
    cycle_mult,
    order_mult,
    turns,
    orders,
    beam,
    precond,
    inv_spec,
    mix,
    applied,
    sums,
    direction,
    residual,
    noise,
    mask,
    gathered,
    colat,
    azim,
    amps,
    there,
    there_mid,
    arrived,
    turned,
    weighted,
    home,
    home_mid,
    returned,
    flipped,
    combined,
    parts,
    totals,
    sum_y,
    sum_z,
    sum_x,
    load_sem,
    gather_send,
    gather_recv,
    z_send,
    z_recv,
    y_send,
    y_recv,
    x_send,
    x_recv,
    sum_send,
    sum_recv,
):
    x_me = lax.axis_index("band")
    z_me = lax.axis_index("blk_0")
    y_me = lax.axis_index("blk_1") * 2 + lax.axis_index("blk_2")
    right, left, across = (lax.rem(x_me + off, 4) for off in (1, 3, 2))
    z_others = [lax.rem(z_me + off, 8) for off in range(1, 8)]
    y_others = [lax.rem(y_me + off, 8) for off in range(1, 8)]

    def at_x(index):
        return {"band": index}

    def at_z(index):
        return {"blk_0": index}

    def at_y(index):
        return {"blk_1": lax.div(index, 2), "blk_2": lax.rem(index, 2)}

    peers = [at_x(i) for i in (right, left, across)]
    peers += [at_z(i) for i in z_others] + [at_y(i) for i in y_others]
    barrier = pltpu.get_barrier_semaphore()
    for peer in peers:
        pl.semaphore_signal(barrier, inc=1, device_id=peer, device_id_type=MESH)

    loads = [
        pltpu.make_async_copy(source, target, load_sem.at[index])
        for index, (source, target) in enumerate(
            ((direction_in, direction), (mask_in, mask), (noise_in, noise), (residual_in, residual))
        )
    ]
    for load in loads:
        load.start()

    sent = []

    def send(source, target, send_sem, recv_sem, peer):
        copy = pltpu.make_async_remote_copy(
            src_ref=source,
            dst_ref=target,
            send_sem=send_sem,
            recv_sem=recv_sem,
            device_id=peer,
            device_id_type=MESH,
        )
        copy.start()
        sent.append(copy)
        return copy

    def arrive(copies):
        for copy in copies:
            copy.wait_recv()

    loads[0].wait()
    for s in range(STOKES):
        for k in range(2):
            for c in range(COMP):
                gathered[s, x_me, k, c] = direction[c * 3 + s, k].astype(BF16)
        if s == 0:
            pl.semaphore_wait(barrier, len(peers))
        if s == 0:
            direct = []
        direct.append(
            [
                send(
                    gathered.at[s, x_me],
                    gathered.at[s, x_me],
                    gather_send.at[s, way],
                    gather_recv.at[s, way],
                    at_x(peer),
                )
                for way, peer in enumerate((right, left))
            ]
        )

    def forward_on(s):
        arrive(direct[s])
        return [
            send(
                gathered.at[s, source, way],
                gathered.at[s, source, way],
                gather_send.at[s, 2 + way],
                gather_recv.at[s, 2 + way],
                at_x(peer),
            )
            for way, (source, peer) in enumerate(((left, right), (right, left)))
        ]

    def make_colat():
        @pl.loop(0, CYCLES // 32)
        def _(block):
            rows = pl.ds(pl.multiple_of(block * 32, 32), 32)

            def put(tile, value):
                colat[rows, tile * 128 : (tile + 1) * 128] = value

            colat_rows(cycle_mult[rows, :], put)

    def make_azim():
        @pl.loop(0, BLOCKS)
        def _(block):
            rows = pl.ds(pl.multiple_of(block * 32, 32), 32)
            real_rows = pl.ds(pl.multiple_of(block * 64, 32), 32)
            imag_rows = pl.ds(pl.multiple_of(block * 64 + 32, 32), 32)

            def put(tile, real, imag):
                azim[real_rows, tile * 128 : (tile + 1) * 128] = real
                azim[imag_rows, tile * 128 : (tile + 1) * 128] = imag

            azim_rows(order_mult[rows, :], put)

    lane = lax.broadcasted_iota(jnp.int32, (R_DEV, 128), 1)
    on_left = lane < 64
    on_left8 = on_left[:8]
    low = (lane & 63) < 32

    def legendre(s):
        @pl.loop(0, L // 256)
        def _(block):
            first = pl.multiple_of(block * 256, 256)
            piece = block // 2
            inner = pl.ds(pl.multiple_of((block % 2) * 256, 256), 256)
            triangle = at_least(orders[:, 0:1], first, 256)
            for k in range(2):
                comps = [gathered[s, piece, k, c, :, inner].astype(F32) for c in range(COMP)]
                for x in range(SLOTS):
                    mixed = mix[x, 0] * comps[0]
                    for c in range(1, COMP):
                        mixed = mixed + mix[x, c] * comps[c]
                    row = (x * 2 + k) * M_DEV
                    value = mixed * beam[x : x + 1, pl.ds(first, 256)] * triangle
                    amps[row : row + M_DEV, pl.ds(first, 256)] = value.astype(BF16)

        @pl.loop(0, CYCLES // 256)
        def _(block):
            rows = pl.ds(pl.multiple_of(block * 256, 256), 256)
            side = lax.dot_general(colat[rows, :], amps[...], NT, preferred_element_type=F32)
            main = side[:, :128].reshape(2, 8, 16, 128)
            tail = side[:, 128:].reshape(16, 16, 128)
            wide = lax.broadcasted_iota(jnp.int32, (128, 128), 1) < 64
            packed = jnp.where(
                wide,
                tail[:, :8].reshape(128, 128),
                pltpu.roll(tail[:, 8:].reshape(128, 128), 64, 1),
            )
            there[s, pl.ds(block * 2, 2), :, 0:16, :] = main.astype(BF16)
            there[s, pl.ds(block * 2, 2), :, 16:24, :] = packed.reshape(2, 8, 8, 128).astype(BF16)

    def start_z(way, s, source, middle):
        copies = [
            send(
                source.at[s, other],
                middle.at[s, z_me],
                z_send.at[way, s, index],
                z_recv.at[way, s, index],
                at_z(other),
            )
            for index, other in enumerate(z_others)
        ]
        middle[s, z_me] = source[s, z_me]
        return copies

    def start_y(way, s, middle, target):
        copies = [
            send(
                middle.at[s, :, other],
                target.at[s, :, y_me],
                y_send.at[way, s, index],
                y_recv.at[way, s, index],
                at_y(other),
            )
            for index, other in enumerate(y_others)
        ]
        target[s, :, y_me] = middle[s, :, y_me]
        return copies

    def azimuth(s):
        @pl.loop(0, BLOCKS // 2)
        def _(tile):
            cols = pl.ds(pl.multiple_of(tile * 128, 128), 128)
            sign, cosine, sine = turns[0:1, cols], turns[1:2, cols], turns[2:3, cols]
            plane, place = tile // 4, (tile % 4) * 2
            first = arrived[s, plane, place, 0:16, :].astype(F32)
            second = arrived[s, plane, place + 1, 0:16, :].astype(F32)
            third = arrived[s, plane, place, 16:24, :].astype(F32)
            fourth = arrived[s, plane, place + 1, 16:24, :].astype(F32)
            values = [
                jnp.where(on_left, first, pltpu.roll(second, 64, 1)),
                jnp.where(on_left, pltpu.roll(first, 64, 1), second),
                jnp.concatenate(
                    [
                        jnp.where(on_left8, third, pltpu.roll(fourth, 64, 1)),
                        jnp.where(on_left8, pltpu.roll(third, 64, 1), fourth),
                    ],
                    axis=0,
                ),
            ]
            for x, value in enumerate(values):
                straight = cosine * value
                crossed = sine * partner(value, low)
                for q, part in enumerate(
                    (value, straight - crossed, sign * value, straight + crossed)
                ):
                    row = q * 48 + x * R_DEV
                    turned[row : row + R_DEV, cols] = part.astype(BF16)

        @pl.loop(0, QUARTER // 256)
        def _(block):
            start = pl.multiple_of(block * 256, 256)
            cols = pl.ds(start, 256)
            sky = lax.dot_general(turned[...], azim[:, cols], NN, preferred_element_type=F32)
            for q in range(4):
                cells = pl.ds(pl.multiple_of(q * QUARTER + start, 256), 256)
                keep = mask[:, cells].astype(F32)
                for x in range(SLOTS):
                    row = q * 48 + x * R_DEV
                    weight = noise[x, s, :, cells] * keep
                    weighted[row : row + R_DEV, cols] = (
                        weight * sky[row : row + R_DEV, :]
                    ).astype(BF16)

        @pl.loop(0, BLOCKS // 4)
        def _(block):
            rows = pl.ds(pl.multiple_of(block * 256, 256), 256)
            back = lax.dot_general(weighted[...], azim[rows, :], NT, preferred_element_type=F32)
            for sub in range(2):
                tile = block * 2 + sub
                cols = pl.ds(pl.multiple_of(tile * 128, 128), 128)
                sign, cosine, sine = turns[0:1, cols], turns[1:2, cols], turns[2:3, cols]
                lanes = slice(sub * 128, sub * 128 + 128)
                values = []
                for x in range(SLOTS):
                    b0, b1, b2, b3 = (
                        back[q * 48 + x * R_DEV : q * 48 + x * R_DEV + R_DEV, lanes]
                        for q in range(4)
                    )
                    values.append(
                        b0 + sign * b2 + cosine * (b1 + b3) + sine * partner(b1 - b3, low)
                    )
                zero, one, two = values
                plane, place = tile // 4, (tile % 4) * 2
                home[s, plane, place, 0:16, :] = jnp.where(
                    on_left, zero, pltpu.roll(one, 64, 1)
                ).astype(BF16)
                home[s, plane, place + 1, 0:16, :] = jnp.where(
                    on_left, pltpu.roll(zero, 64, 1), one
                ).astype(BF16)
                home[s, plane, place, 16:24, :] = jnp.where(
                    on_left8, two[:8], pltpu.roll(two[8:], 64, 1)
                ).astype(BF16)
                home[s, plane, place + 1, 16:24, :] = jnp.where(
                    on_left8, pltpu.roll(two[:8], 64, 1), two[8:]
                ).astype(BF16)

    def legendre_back(s):
        @pl.loop(0, 8)
        def _(plane):
            cols = pl.ds(pl.multiple_of(plane * 128, 128), 128)
            main = returned[s, plane, :, 0:16, :].astype(F32).reshape(128, 128)
            tail = returned[s, plane, :, 16:24, :].astype(F32)
            swapped = pltpu.roll(tail.reshape(64, 128), 64, 1).reshape(8, 8, 128)
            both = jnp.concatenate([tail, swapped], axis=1).reshape(128, 128)
            flipped[0:128, cols] = main.T.astype(BF16)
            flipped[128:256, cols] = both.T.astype(BF16)

        @pl.loop(0, L // 256)
        def _(block):
            start = pl.multiple_of(block * 256, 256)
            cols = pl.ds(start, 256)
            harm = lax.dot_general(
                flipped[0:192, :], colat[:, cols], NN, preferred_element_type=F32
            )
            triangle = at_least(orders[:, 0:1], start, 256)
            piece = block // 2
            inner = pl.ds(pl.multiple_of((block % 2) * 256, 256), 256)
            for k in range(2):
                shaped = []
                for x in range(SLOTS):
                    row = (x * 2 + k) * M_DEV
                    shaped.append(harm[row : row + M_DEV, :] * beam[x : x + 1, cols] * triangle)
                for c in range(COMP):
                    total = mix[0, c] * shaped[0]
                    for x in range(1, SLOTS):
                        total = total + mix[x, c] * shaped[x]
                    combined[s, piece, c, k, :, inner] = total.astype(BF16)

    def start_x(s):
        return [
            send(
                combined.at[s, other],
                parts.at[s, index],
                x_send.at[s, index],
                x_recv.at[s, index],
                at_x(other),
            )
            for index, other in enumerate((right, left, across))
        ]

    def apply(s):
        for c in range(COMP):
            field = c * 3 + s
            pre = precond[field : field + 1, :]
            prior = inv_spec[field : field + 1, :]
            for k in range(2):
                total = combined[s, x_me, c, k].astype(F32)
                for index in range(3):
                    total = total + parts[s, index, c, k].astype(F32)
                dir_now = direction[field, k]
                res_now = residual[field, k]
                value = prior * dir_now + total
                applied[field, k] = value
                scaled = pre * res_now
                totals[0] += folded(res_now * scaled)
                totals[1] += folded(dir_now * value)
                totals[2] += folded(value * scaled)
                totals[3] += folded(value * pre * value)

    def sum_over(stage, buffer, me, others, place, value):
        buffer[me] = value
        copies = [
            send(
                buffer.at[me],
                buffer.at[me],
                sum_send.at[stage, index],
                sum_recv.at[stage, index],
                place(other),
            )
            for index, other in enumerate(others)
        ]
        arrive(copies)
        return jnp.sum(buffer[...], axis=0)

    totals[...] = jnp.zeros_like(totals)
    amps[192:256, :] = jnp.zeros((64, L), BF16)
    make_colat()
    relayed = [forward_on(0)]
    for load in loads[1:]:
        load.wait()
    arrive(relayed[0])
    legendre(0)
    z_there = [start_z(0, 0, there, there_mid)]
    relayed.append(forward_on(1))
    make_azim()
    relayed.append(forward_on(2))
    arrive(relayed[1])
    legendre(1)
    z_there.append(start_z(0, 1, there, there_mid))
    arrive(z_there[0])
    y_there = [start_y(0, 0, there_mid, arrived)]
    arrive(relayed[2])
    legendre(2)
    z_there.append(start_z(0, 2, there, there_mid))
    arrive(y_there[0])
    azimuth(0)
    z_home = [start_z(1, 0, home, home_mid)]
    arrive(z_there[1])
    y_there.append(start_y(0, 1, there_mid, arrived))
    arrive(y_there[1])
    azimuth(1)
    z_home.append(start_z(1, 1, home, home_mid))
    arrive(z_there[2])
    y_there.append(start_y(0, 2, there_mid, arrived))
    arrive(y_there[2])
    azimuth(2)
    z_home.append(start_z(1, 2, home, home_mid))
    arrive(z_home[0])
    y_home = [start_y(1, 0, home_mid, returned)]
    arrive(y_home[0])
    legendre_back(0)
    x_home = [start_x(0)]
    arrive(z_home[1])
    y_home.append(start_y(1, 1, home_mid, returned))
    arrive(y_home[1])
    legendre_back(1)
    x_home.append(start_x(1))
    arrive(z_home[2])
    y_home.append(start_y(1, 2, home_mid, returned))
    arrive(x_home[0])
    apply(0)
    arrive(y_home[2])
    legendre_back(2)
    x_home.append(start_x(2))
    arrive(x_home[1])
    apply(1)
    arrive(x_home[2])
    apply(2)

    row = lax.broadcasted_iota(jnp.int32, (8, 128), 0)
    value = jnp.zeros((8, 128), F32)
    for index in range(4):
        value = jnp.where(row == index, jnp.sum(totals[index], axis=0, keepdims=True), value)
    value = sum_over(0, sum_y, y_me, y_others, at_y, value)
    value = sum_over(1, sum_z, z_me, z_others, at_z, value)
    value = sum_over(2, sum_x, x_me, (right, left, across), at_x, value)
    sums[...] = jnp.broadcast_to(jnp.sum(value, axis=1, keepdims=True), (8, 128))
    for copy in sent:
        copy.wait_send()


def operator(direction, residual, noise, mask, *small):
    dma = pltpu.SemaphoreType.DMA
    block = (STOKES, 8, 8, 24, 128)
    local = (FIELDS, 2, M_DEV, L_DEV)
    return pl.pallas_call(
        operator_kernel,
        in_specs=[pl.BlockSpec(memory_space=pl.ANY)] * 4 + [in_vmem()] * 7 + [in_smem()],
        out_specs=[in_vmem(), in_vmem()],
        out_shape=[jax.ShapeDtypeStruct(local, F32), jax.ShapeDtypeStruct((8, 128), F32)],
        scratch_shapes=[
            VMEM(local, F32),
            VMEM(local, F32),
            VMEM((SLOTS, STOKES, R_DEV, PHI), F32),
            VMEM((R_DEV, PHI), jnp.int32),
            VMEM((STOKES, 4, 2, COMP, M_DEV, L_DEV), BF16),
            VMEM((CYCLES, L), BF16),
            VMEM((2 * MODES, QUARTER), BF16),
            VMEM((256, L), BF16),
            VMEM(block, BF16),
            VMEM(block, BF16),
            VMEM(block, BF16),
            VMEM((192, 2 * MODES), BF16),
            VMEM((192, QUARTER), BF16),
            VMEM(block, BF16),
            VMEM(block, BF16),
            VMEM(block, BF16),
            VMEM((256, CYCLES), BF16),
            VMEM((STOKES, 4, COMP, 2, M_DEV, L_DEV), BF16),
            VMEM((STOKES, 3, COMP, 2, M_DEV, L_DEV), BF16),
            VMEM((4, 8, 128), F32),
            VMEM((8, 8, 128), F32),
            VMEM((8, 8, 128), F32),
            VMEM((4, 8, 128), F32),
            dma((4,)),
            dma((STOKES, 4)),
            dma((STOKES, 4)),
            dma((2, STOKES, 7)),
            dma((2, STOKES, 7)),
            dma((2, STOKES, 7)),
            dma((2, STOKES, 7)),
            dma((STOKES, 3)),
            dma((STOKES, 3)),
            dma((3, 7)),
            dma((3, 7)),
        ],
        compiler_params=pltpu.CompilerParams(
            collective_id=0, has_side_effects=True, vmem_limit_bytes=60 * 1024 * 1024
        ),
        name="operator",
    )(direction, residual, noise, mask, *small)


def slot_tables(my_slots, mixing, beams):
    select = (my_slots[:, None] == jnp.arange(BANDS, dtype=jnp.int32)[None, :]).astype(F32)
    highest = lax.Precision.HIGHEST
    return (jnp.dot(select, mixing, precision=highest), jnp.dot(select, beams, precision=highest))


def quarter_turns(m_order):
    m_lane = jnp.broadcast_to(m_order.reshape(BLOCKS, 1, M_DEV), (BLOCKS, 2, M_DEV))
    part = jnp.array([1.0, -1.0], F32)[None, :, None]
    phase = m_lane % 4
    sign = jnp.where(phase % 2 == 0, 1.0, -1.0).astype(F32)
    cosine = jnp.where(phase == 0, 1.0, jnp.where(phase == 2, -1.0, 0.0)).astype(F32)
    sine = jnp.where(phase == 1, 1.0, jnp.where(phase == 3, -1.0, 0.0)).astype(F32) * part
    rows = jnp.stack([sign, cosine, sine]).reshape(3, 2 * MODES)
    return jnp.concatenate([rows, jnp.zeros((5, 2 * MODES), F32)])


def on_device(
    solution,
    residual,
    direction,
    precond,
    inv_spec,
    mixing,
    beams,
    slot_band,
    m_order,
    cycle_order,
    inv_noise,
    pix_mask,
):
    band_index = lax.axis_index("band")
    block_index = lax.axis_index(BLK)
    cycle_mult = jnp.broadcast_to((2 * cycle_order + 1)[:, None], (CYCLES, 128))
    order_mult = jnp.broadcast_to(m_order[:, None], (MODES, 128))
    turns = quarter_turns(m_order)
    my_orders = lax.dynamic_slice_in_dim(m_order, block_index * M_DEV, M_DEV)
    orders = jnp.broadcast_to(my_orders[:, None], (M_DEV, 128))
    my_slots = lax.dynamic_slice_in_dim(slot_band, band_index * SLOTS, SLOTS)
    slot_mix, slot_beam = slot_tables(my_slots, mixing, beams)
    applied, sums = operator(
        direction,
        residual,
        inv_noise,
        pix_mask,
        cycle_mult,
        order_mult,
        turns,
        orders,
        slot_beam,
        precond,
        inv_spec,
        slot_mix,
    )
    precond_full = precond[:, None, None, :]
    norm_old, curvature, crossed, squared = (sums[index, 0] for index in range(4))
    step_size = norm_old / curvature
    solution_next = solution + step_size * direction
    residual_next = residual - step_size * applied
    scaled_next = precond_full * residual_next
    norm_new = norm_old - 2.0 * step_size * crossed + step_size * step_size * squared
    direction_next = scaled_next + norm_new / norm_old * direction
    return (solution_next, residual_next, direction_next)


def solution(mesh):
    finer = Mesh(
        mesh.devices.reshape(mesh.shape["band"], 8, 4, 2), ("band", "blk_0", "blk_1", "blk_2")
    )
    in_specs = (
        P(None, None, BLK, "band"),
        P(None, None, BLK, "band"),
        P(None, None, BLK, "band"),
        P(None, "band"),
        P(None, "band"),
        P(),
        P(),
        P(),
        P(),
        P(),
        P("band", None, BLK, None),
        P(BLK, None),
    )
    out_specs = (P(None, None, BLK, "band"), P(None, None, BLK, "band"), P(None, None, BLK, "band"))
    return jax.shard_map(
        on_device, mesh=finer, in_specs=in_specs, out_specs=out_specs, check_vma=False
    )
```

```python
import math

import jax
import jax.numpy as jnp
from jax import lax
from jax.experimental import pallas as pl
from jax.experimental.pallas import tpu as pltpu
from jax.sharding import Mesh
from jax.sharding import PartitionSpec as P

COMP = 3
STOKES = 3
FIELDS = 9
BANDS = 9
SLOTS = 3
L = 2048
CYCLES = 1024
MODES = 2048
PHI = 4096
QUARTER = PHI // 4
M_DEV = 32
R_DEV = 16
BLOCKS = 64
L_DEV = 512
BLK = ("blk_0", "blk_1", "blk_2")
SCALE = 1.0 / math.sqrt(2048)
VMEM = pltpu.VMEM
MESH = pl.DeviceIdType.MESH
F32 = jnp.float32
BF16 = jnp.bfloat16
NT = (((1,), (1,)), ((), ()))
NN = (((1,), (0,)), ((), ()))


def in_vmem():
    return pl.BlockSpec(memory_space=VMEM)


def in_smem():
    return pl.BlockSpec(memory_space=pltpu.SMEM)


def unit_circle(turn):
    half = (((turn + 2048) & 4095) - 2048).astype(F32) * (math.pi / 4096)
    sq = half * half
    sine = half * (
        1
        + sq
        * (-1 / 6 + sq * (1 / 120 + sq * (-1 / 5040 + sq * (1 / 362880 + sq * (-1 / 39916800)))))
    )
    cosine = 1 + sq * (
        -1 / 2
        + sq
        * (
            1 / 24
            + sq * (-1 / 720 + sq * (1 / 40320 + sq * (-1 / 3628800 + sq * (1 / 479001600))))
        )
    )
    return cosine * cosine - sine * sine, 2 * sine * cosine


def first_turns(mult):
    lane = lax.broadcasted_iota(jnp.int32, mult.shape, 1)
    cosine, sine = unit_circle((mult * lane) & 4095)
    step_cos, step_sin = unit_circle((mult * 128) & 4095)
    return cosine * SCALE, sine * SCALE, step_cos, step_sin


def colat_rows(mult, store):
    cosine, sine, step_cos, step_sin = first_turns(mult)
    for tile in range(L // 128):
        store(tile, cosine.astype(BF16))
        cosine, sine = cosine * step_cos - sine * step_sin, sine * step_cos + cosine * step_sin


def azim_rows(mult, store):
    cosine, sine, step_cos, step_sin = first_turns(mult)
    for tile in range(QUARTER // 128):
        store(tile, cosine.astype(BF16), (-sine).astype(BF16))
        cosine, sine = cosine * step_cos - sine * step_sin, sine * step_cos + cosine * step_sin


STEP = 32


def azim_columns(order, first_turn, store):
    cell = lax.broadcasted_iota(jnp.int32, (STEP, 128), 0)
    cosine, sine = unit_circle((order * cell + first_turn) & 4095)
    step_cos, step_sin = unit_circle((order * STEP) & 4095)
    cosine, sine = cosine * SCALE, sine * SCALE
    for step in range(QUARTER // STEP):
        store(step, cosine.astype(BF16))
        cosine, sine = cosine * step_cos - sine * step_sin, sine * step_cos + cosine * step_sin


def spread(values, row):
    line = values[pl.ds(row, 1), :].astype(F32)
    return jnp.broadcast_to(line, (128, 128)).T.astype(jnp.int32)


def at_least(orders, first):
    l_values = first + lax.broadcasted_iota(jnp.int32, (M_DEV, 256), 1)
    return (l_values >= jnp.concatenate([orders, orders], axis=1)).astype(F32)


def partner(value, low):
    return jnp.where(low, pltpu.roll(value, 96, 1), pltpu.roll(value, 32, 1))


def folded(value):
    tiles = [
        value[8 * i : 8 * i + 8, 128 * j : 128 * j + 128]
        for i in range(value.shape[0] // 8)
        for j in range(value.shape[1] // 128)
    ]
    while len(tiles) > 1:
        tiles = [first + second for first, second in zip(tiles[::2], tiles[1::2])]
    return tiles[0]


def operator_kernel(
    direction_in,
    residual_in,
    noise_in,
    mask_in,
    m_rows,
    cycle_rows,
    beams,
    precond,
    inv_spec,
    mixing,
    slot_band,
    applied,
    sums,
    direction,
    residual,
    noise,
    mask,
    gathered,
    colat,
    azim,
    azim_across,
    turns,
    order_lanes,
    orders,
    beam,
    amps,
    there,
    there_mid,
    arrived,
    turned,
    weighted,
    home,
    home_mid,
    returned,
    flipped,
    combined,
    parts,
    totals,
    sum_y,
    sum_z,
    sum_x,
    load_sem,
    gather_send,
    gather_recv,
    z_send,
    z_recv,
    y_send,
    y_recv,
    x_send,
    x_recv,
    sum_send,
    sum_recv,
):
    x_me = lax.axis_index("band")
    z_me = lax.axis_index("blk_0")
    y_me = lax.axis_index("blk_1") * 2 + lax.axis_index("blk_2")
    right, left, across = (lax.rem(x_me + off, 4) for off in (1, 3, 2))
    z_others = [lax.rem(z_me + off, 8) for off in range(1, 8)]
    y_others = [lax.rem(y_me + off, 8) for off in range(1, 8)]

    def at_x(index):
        return {"band": index}

    def at_z(index):
        return {"blk_0": index}

    def at_y(index):
        return {"blk_1": lax.div(index, 2), "blk_2": lax.rem(index, 2)}

    peers = [at_x(i) for i in (right, left, across)]
    peers += [at_z(i) for i in z_others] + [at_y(i) for i in y_others]
    barrier = pltpu.get_barrier_semaphore()
    for peer in peers:
        pl.semaphore_signal(barrier, inc=1, device_id=peer, device_id_type=MESH)

    loads = [
        pltpu.make_async_copy(source, target, load_sem.at[index])
        for index, (source, target) in enumerate(
            ((direction_in, direction), (mask_in, mask), (noise_in, noise), (residual_in, residual))
        )
    ]
    for load in loads:
        load.start()

    sent = []

    def describe(source, target, send_sem, recv_sem, peer):
        return pltpu.make_async_remote_copy(
            src_ref=source,
            dst_ref=target,
            send_sem=send_sem,
            recv_sem=recv_sem,
            device_id=peer,
            device_id_type=MESH,
        )

    def send(*ends):
        copy = describe(*ends)
        copy.start()
        sent.append(copy)
        return copy

    def arrive(copies):
        for copy in copies:
            copy.wait_recv()

    def halve(s):
        for k in range(2):
            for c in range(COMP):
                gathered[s, x_me, k, c] = direction[c * 3 + s, k].astype(BF16)

    def gather(s):
        return [
            send(
                gathered.at[s, x_me],
                gathered.at[s, x_me],
                gather_send.at[s, way],
                gather_recv.at[s, way],
                at_x(peer),
            )
            for way, peer in enumerate((right, left))
        ]

    def forward_on(s):
        return [
            send(
                gathered.at[s, source, way],
                gathered.at[s, source, way],
                gather_send.at[s, 2 + way],
                gather_recv.at[s, 2 + way],
                at_x(peer),
            )
            for way, (source, peer) in enumerate(((left, right), (right, left)))
        ]

    def make_colat():
        @pl.loop(0, CYCLES // 128)
        def _(block):
            mult = 2 * spread(cycle_rows, block) + 1
            for sub in range(4):
                rows = pl.ds(pl.multiple_of(block * 128 + sub * 32, 32), 32)

                def put(tile, value):
                    colat[rows, tile * 128 : (tile + 1) * 128] = value

                colat_rows(mult[sub * 32 : sub * 32 + 32], put)

    def make_azim(begin, end):
        @pl.loop(begin, end)
        def _(block):
            mult = spread(m_rows, block)
            for sub in range(4):
                first = block * 256 + sub * 64
                real_rows = pl.ds(pl.multiple_of(first, 32), 32)
                imag_rows = pl.ds(pl.multiple_of(first + 32, 32), 32)

                def put(tile, real, imag):
                    azim[real_rows, tile * 128 : (tile + 1) * 128] = real
                    azim[imag_rows, tile * 128 : (tile + 1) * 128] = imag

                azim_rows(mult[sub * 32 : sub * 32 + 32], put)

    def make_azim_across(begin, end):
        @pl.loop(begin, end)
        def _(tile):
            cols = pl.ds(pl.multiple_of(tile * 128, 128), 128)
            order = order_lanes[tile % 2, pl.ds(tile // 2, 1), :]
            part = lax.broadcasted_iota(jnp.int32, (1, 128), 1) & 32

            def put(step, value):
                azim_across[step * STEP : (step + 1) * STEP, cols] = value

            azim_columns(order, part * 32, put)

    mix = [[None] * COMP for _ in range(SLOTS)]
    for x in range(SLOTS):
        slot = slot_band[x_me * SLOTS + x]
        for c in range(COMP):
            mix[x][c] = jnp.where(slot < BANDS, mixing[jnp.minimum(slot, BANDS - 1), c], 0.0)

    def make_small():
        place = lax.broadcasted_iota(jnp.int32, (16, 128), 1)
        line = m_rows[...]
        even = jnp.where(
            place < 32, line, jnp.where(place < 96, pltpu.roll(line, 32, 1), pltpu.roll(line, 64, 1))
        )
        odd = jnp.where(
            place < 32, pltpu.roll(line, 64, 1), jnp.where(place < 96, pltpu.roll(line, 96, 1), line)
        )
        way = jnp.where((place & 63) < 32, 1.0, -1.0)
        for parity, value in enumerate((even, odd)):
            order_lanes[parity] = value
            phase = value & 3
            turns[0, parity] = jnp.where((value & 1) == 0, 1.0, -1.0)
            turns[1, parity] = jnp.where(phase == 0, 1.0, jnp.where(phase == 2, -1.0, 0.0))
            turns[2, parity] = way * jnp.where(
                phase == 1, 1.0, jnp.where(phase == 3, -1.0, 0.0)
            )
        for x in range(SLOTS):
            slot = slot_band[x_me * SLOTS + x]
            total = jnp.zeros((1, L), F32)
            for band in range(BANDS):
                total = jnp.where(slot == band, beams[band : band + 1, :], total)
            beam[x : x + 1, :] = total
        blk = z_me * 8 + y_me
        all_orders = spread(m_rows, lax.div(blk, 4))
        for sub in range(4):

            @pl.when(lax.rem(blk, 4) == sub)
            def _():
                orders[...] = all_orders[sub * 32 : sub * 32 + 32]

    def turns_of(tile):
        return [turns[index, tile % 2, pl.ds(tile // 2, 1), :] for index in range(3)]

    lane = lax.broadcasted_iota(jnp.int32, (R_DEV, 128), 1)
    on_left = lane < 64
    on_left8 = on_left[:8]
    low = (lane & 63) < 32

    def legendre(s):
        @pl.loop(0, L // 256)
        def _(block):
            first = pl.multiple_of(block * 256, 256)
            piece = block // 2
            inner = pl.ds(pl.multiple_of((block % 2) * 256, 256), 256)
            triangle = at_least(orders[...], first)
            for k in range(2):
                comps = [gathered[s, piece, k, c, :, inner].astype(F32) for c in range(COMP)]
                for x in range(SLOTS):
                    mixed = mix[x][0] * comps[0]
                    for c in range(1, COMP):
                        mixed = mixed + mix[x][c] * comps[c]
                    row = (x * 2 + k) * M_DEV
                    value = mixed * beam[x : x + 1, pl.ds(first, 256)] * triangle
                    amps[row : row + M_DEV, pl.ds(first, 256)] = value.astype(BF16)

        @pl.loop(0, CYCLES // 256)
        def _(block):
            rows = pl.ds(pl.multiple_of(block * 256, 256), 256)
            side = lax.dot_general(colat[rows, :], amps[...], NT, preferred_element_type=F32)
            main = side[:, :128].reshape(2, 8, 16, 128)
            tail = side[:, 128:].reshape(16, 16, 128)
            wide = lax.broadcasted_iota(jnp.int32, (128, 128), 1) < 64
            packed = jnp.where(
                wide,
                tail[:, :8].reshape(128, 128),
                pltpu.roll(tail[:, 8:].reshape(128, 128), 64, 1),
            )
            there[s, pl.ds(block * 2, 2), :, 0:16, :] = main.astype(BF16)
            there[s, pl.ds(block * 2, 2), :, 16:24, :] = packed.reshape(2, 8, 8, 128).astype(BF16)

    def z_copy(way, s, off, source, middle):
        other = lax.rem(z_me + off, 8)
        return describe(
            source.at[s, other],
            middle.at[s, z_me],
            z_send.at[way, s, off - 1],
            z_recv.at[way, s, off - 1],
            at_z(other),
        )

    def start_z(way, s, source, middle):
        for off in (1, 7, 2, 6, 3, 5, 4):
            z_copy(way, s, off, source, middle).start()

    def y_copy(way, s, index, source, target):
        return describe(
            source, target, y_send.at[way, s, index], y_recv.at[way, s, index], at_y(y_others[index])
        )

    def pass_on(way, s, source, middle, target):
        for off in (0, 1, 7, 2, 6, 3, 5, 4):
            plane = lax.rem(z_me + 8 - off, 8)
            held = source if off == 0 else middle
            if off:
                copy = z_copy(way, s, off, source, middle)
                copy.wait_recv()
                sent.append(copy)
            for index, other in enumerate(y_others):
                y_copy(
                    way, s, index, held.at[s, plane, other], target.at[s, plane, y_me]
                ).start()
            target[s, plane, y_me] = held[s, plane, y_me]

    def wait_y(way, s, middle, target):
        for index, other in enumerate(y_others):
            copy = y_copy(way, s, index, middle.at[s, :, other], target.at[s, :, y_me])
            copy.wait_recv()
            sent.append(copy)

    def azimuth(s):
        @pl.loop(0, BLOCKS // 2, unroll=4)
        def _(tile):
            cols = pl.ds(pl.multiple_of(tile * 128, 128), 128)
            sign, cosine, sine = turns_of(tile)
            plane, place = tile // 4, (tile % 4) * 2
            first = arrived[s, plane, place, 0:16, :].astype(F32)
            second = arrived[s, plane, place + 1, 0:16, :].astype(F32)
            third = arrived[s, plane, place, 16:24, :].astype(F32)
            fourth = arrived[s, plane, place + 1, 16:24, :].astype(F32)
            values = [
                jnp.where(on_left, first, pltpu.roll(second, 64, 1)),
                jnp.where(on_left, pltpu.roll(first, 64, 1), second),
                jnp.concatenate(
                    [
                        jnp.where(on_left8, third, pltpu.roll(fourth, 64, 1)),
                        jnp.where(on_left8, pltpu.roll(third, 64, 1), fourth),
                    ],
                    axis=0,
                ),
            ]
            for x, value in enumerate(values):
                straight = cosine * value
                crossed = sine * partner(value, low)
                for q, part in enumerate(
                    (value, straight - crossed, sign * value, straight + crossed)
                ):
                    row = q * 48 + x * R_DEV
                    turned[row : row + R_DEV, cols] = part.astype(BF16)

        @pl.loop(0, QUARTER // 256)
        def _(block):
            start = pl.multiple_of(block * 256, 256)
            cols = pl.ds(start, 256)
            sky = lax.dot_general(turned[...], azim[:, cols], NN, preferred_element_type=F32)
            for q in range(4):
                cells = pl.ds(pl.multiple_of(q * QUARTER + start, 256), 256)
                keep = mask[:, cells].astype(F32)
                for x in range(SLOTS):
                    row = q * 48 + x * R_DEV
                    weight = noise[x, s, :, cells] * keep
                    weighted[row : row + R_DEV, cols] = (
                        weight * sky[row : row + R_DEV, :]
                    ).astype(BF16)

        @pl.loop(1, 9)
        def _(off):
            home_plane = lax.rem(z_me + off, 8)
            backs = []
            for half in range(2):
                cols = pl.ds(pl.multiple_of(home_plane * 512 + half * 256, 256), 256)
                backs.append(
                    lax.dot_general(
                        weighted[...], azim_across[:, cols], NN, preferred_element_type=F32
                    )
                )
            for inner in range(4):
                tile = home_plane * 4 + inner
                back, sub = backs[inner // 2], inner % 2
                sign, cosine, sine = turns_of(tile)
                lanes = slice(sub * 128, sub * 128 + 128)
                values = []
                for x in range(SLOTS):
                    b0, b1, b2, b3 = (
                        back[q * 48 + x * R_DEV : q * 48 + x * R_DEV + R_DEV, lanes]
                        for q in range(4)
                    )
                    values.append(
                        b0 + sign * b2 + cosine * (b1 + b3) + sine * partner(b1 - b3, low)
                    )
                zero, one, two = values
                plane, place = home_plane, inner * 2
                home[s, plane, place, 0:16, :] = jnp.where(
                    on_left, zero, pltpu.roll(one, 64, 1)
                ).astype(BF16)
                home[s, plane, place + 1, 0:16, :] = jnp.where(
                    on_left, pltpu.roll(zero, 64, 1), one
                ).astype(BF16)
                home[s, plane, place, 16:24, :] = jnp.where(
                    on_left8, two[:8], pltpu.roll(two[8:], 64, 1)
                ).astype(BF16)
                home[s, plane, place + 1, 16:24, :] = jnp.where(
                    on_left8, pltpu.roll(two[:8], 64, 1), two[8:]
                ).astype(BF16)

            @pl.when(off < 8)
            def _():
                z_copy(1, s, off, home, home_mid).start()

    def legendre_back(s):
        @pl.loop(0, 8)
        def _(plane):
            cols = pl.ds(pl.multiple_of(plane * 128, 128), 128)
            main = returned[s, plane, :, 0:16, :].astype(F32).reshape(128, 128)
            tail = returned[s, plane, :, 16:24, :].astype(F32)
            swapped = pltpu.roll(tail.reshape(64, 128), 64, 1).reshape(8, 8, 128)
            both = jnp.concatenate([tail, swapped], axis=1).reshape(128, 128)
            flipped[0:128, cols] = main.T.astype(BF16)
            flipped[128:256, cols] = both.T.astype(BF16)

        @pl.loop(0, L // 256)
        def _(block):
            start = pl.multiple_of(block * 256, 256)
            cols = pl.ds(start, 256)
            harm = lax.dot_general(
                flipped[0:192, :], colat[:, cols], NN, preferred_element_type=F32
            )
            triangle = at_least(orders[...], start)
            piece = block // 2
            inner = pl.ds(pl.multiple_of((block % 2) * 256, 256), 256)
            for k in range(2):
                shaped = []
                for x in range(SLOTS):
                    row = (x * 2 + k) * M_DEV
                    shaped.append(harm[row : row + M_DEV, :] * beam[x : x + 1, cols] * triangle)
                for c in range(COMP):
                    total = mix[0][c] * shaped[0]
                    for x in range(1, SLOTS):
                        total = total + mix[x][c] * shaped[x]
                    combined[s, piece, c, k, :, inner] = total.astype(BF16)

    def start_x(s):
        return [
            send(
                combined.at[s, other],
                parts.at[s, index],
                x_send.at[s, index],
                x_recv.at[s, index],
                at_x(other),
            )
            for index, other in enumerate((right, left, across))
        ]

    def apply(s):
        for c in range(COMP):
            field = c * 3 + s
            pre = precond[field : field + 1, :]
            prior = inv_spec[field : field + 1, :]
            for k in range(2):
                total = combined[s, x_me, c, k].astype(F32)
                for index in range(3):
                    total = total + parts[s, index, c, k].astype(F32)
                dir_now = direction[field, k]
                res_now = residual[field, k]
                value = prior * dir_now + total
                applied[field, k] = value
                scaled = pre * res_now
                totals[0] += folded(res_now * scaled)
                totals[1] += folded(dir_now * value)
                totals[2] += folded(value * scaled)
                totals[3] += folded(value * pre * value)

    def sum_over(stage, buffer, me, others, place, value):
        buffer[me] = value
        copies = [
            send(
                buffer.at[me],
                buffer.at[me],
                sum_send.at[stage, index],
                sum_recv.at[stage, index],
                place(other),
            )
            for index, other in enumerate(others)
        ]
        arrive(copies)
        return jnp.sum(buffer[...], axis=0)

    loads[0].wait()
    halve(0)
    pl.semaphore_wait(barrier, len(peers))
    direct = gather(0)
    halve(1)
    halve(2)
    totals[...] = jnp.zeros_like(totals)
    amps[192:256, :] = jnp.zeros((64, L), BF16)
    make_small()
    make_colat()
    arrive(direct)
    relayed = forward_on(0)
    direct = gather(1)
    make_azim(0, 8)
    arrive(relayed)
    legendre(0)
    start_z(0, 0, there, there_mid)
    arrive(direct)
    relayed = forward_on(1)
    direct = gather(2)
    make_azim(8, 16)
    arrive(relayed)
    legendre(1)
    start_z(0, 1, there, there_mid)
    arrive(direct)
    relayed = forward_on(2)
    make_azim_across(0, 16)
    pass_on(0, 0, there, there_mid, arrived)
    arrive(relayed)
    legendre(2)
    start_z(0, 2, there, there_mid)
    make_azim_across(16, 32)
    for load in loads[1:]:
        load.wait()
    wait_y(0, 0, there_mid, arrived)
    azimuth(0)
    pass_on(0, 1, there, there_mid, arrived)
    wait_y(0, 1, there_mid, arrived)
    azimuth(1)
    pass_on(0, 2, there, there_mid, arrived)
    wait_y(0, 2, there_mid, arrived)
    azimuth(2)
    pass_on(1, 0, home, home_mid, returned)
    wait_y(1, 0, home_mid, returned)
    legendre_back(0)
    x_home = [start_x(0)]
    pass_on(1, 1, home, home_mid, returned)
    wait_y(1, 1, home_mid, returned)
    legendre_back(1)
    x_home.append(start_x(1))
    arrive(x_home[0])
    apply(0)
    pass_on(1, 2, home, home_mid, returned)
    wait_y(1, 2, home_mid, returned)
    legendre_back(2)
    x_home.append(start_x(2))
    arrive(x_home[1])
    apply(1)
    arrive(x_home[2])
    apply(2)

    row = lax.broadcasted_iota(jnp.int32, (8, 128), 0)
    value = jnp.zeros((8, 128), F32)
    for index in range(4):
        value = jnp.where(row == index, jnp.sum(totals[index], axis=0, keepdims=True), value)
    value = sum_over(0, sum_y, y_me, y_others, at_y, value)
    value = sum_over(1, sum_z, z_me, z_others, at_z, value)
    value = sum_over(2, sum_x, x_me, (right, left, across), at_x, value)
    sums[...] = jnp.broadcast_to(jnp.sum(value, axis=1, keepdims=True), (8, 128))
    for copy in sent:
        copy.wait_send()


def operator(direction, residual, noise, mask, *small):
    dma = pltpu.SemaphoreType.DMA
    block = (STOKES, 8, 8, 24, 128)
    local = (FIELDS, 2, M_DEV, L_DEV)
    return pl.pallas_call(
        operator_kernel,
        in_specs=[pl.BlockSpec(memory_space=pl.ANY)] * 4 + [in_vmem()] * 5 + [in_smem()] * 2,
        out_specs=[in_vmem(), in_vmem()],
        out_shape=[jax.ShapeDtypeStruct(local, F32), jax.ShapeDtypeStruct((8, 128), F32)],
        scratch_shapes=[
            VMEM(local, F32),
            VMEM(local, F32),
            VMEM((SLOTS, STOKES, R_DEV, PHI), F32),
            VMEM((R_DEV, PHI), jnp.int32),
            VMEM((STOKES, 4, 2, COMP, M_DEV, L_DEV), BF16),
            VMEM((CYCLES, L), BF16),
            VMEM((2 * MODES, QUARTER), BF16),
            VMEM((QUARTER, 2 * MODES), BF16),
            VMEM((3, 2, 16, 128), F32),
            VMEM((2, 16, 128), jnp.int32),
            VMEM((M_DEV, 128), jnp.int32),
            VMEM((SLOTS, L), F32),
            VMEM((256, L), BF16),
            VMEM(block, BF16),
            VMEM(block, BF16),
            VMEM(block, BF16),
            VMEM((192, 2 * MODES), BF16),
            VMEM((192, QUARTER), BF16),
            VMEM(block, BF16),
            VMEM(block, BF16),
            VMEM(block, BF16),
            VMEM((256, CYCLES), BF16),
            VMEM((STOKES, 4, COMP, 2, M_DEV, L_DEV), BF16),
            VMEM((STOKES, 3, COMP, 2, M_DEV, L_DEV), BF16),
            VMEM((4, 8, 128), F32),
            VMEM((8, 8, 128), F32),
            VMEM((8, 8, 128), F32),
            VMEM((4, 8, 128), F32),
            dma((4,)),
            dma((STOKES, 4)),
            dma((STOKES, 4)),
            dma((2, STOKES, 7)),
            dma((2, STOKES, 7)),
            dma((2, STOKES, 7)),
            dma((2, STOKES, 7)),
            dma((STOKES, 3)),
            dma((STOKES, 3)),
            dma((3, 7)),
            dma((3, 7)),
        ],
        compiler_params=pltpu.CompilerParams(
            collective_id=0, has_side_effects=True, vmem_limit_bytes=60 * 1024 * 1024
        ),
        name="operator",
    )(direction, residual, noise, mask, *small)


def finish_kernel(sums, precond, solution, residual, direction, applied, out_sol, out_res, out_dir):
    norm_old, curvature, crossed, squared = (
        jnp.concatenate([sums[index : index + 1, :]] * 4, axis=1) for index in range(4)
    )
    step_size = norm_old / curvature
    norm_new = norm_old - 2.0 * step_size * crossed + step_size * step_size * squared
    ratio = norm_new / norm_old
    pre = precond[pl.ds(pl.program_id(0), 1), :]
    for k in range(2):
        dir_now = direction[0, k]
        res_next = residual[0, k] - step_size * applied[0, k]
        out_sol[0, k] = solution[0, k] + step_size * dir_now
        out_res[0, k] = res_next
        out_dir[0, k] = pre * res_next + ratio * dir_now


def finish(sums, precond, *arrays):
    local = (FIELDS, 2, M_DEV, L_DEV)
    field = pl.BlockSpec((1, 2, M_DEV, L_DEV), lambda g: (g, 0, 0, 0))
    whole = [pl.BlockSpec((8, 128), lambda g: (0, 0)), pl.BlockSpec((FIELDS, L_DEV), lambda g: (0, 0))]
    return pl.pallas_call(
        finish_kernel,
        grid=(FIELDS,),
        in_specs=whole + [field] * 4,
        out_specs=[field] * 3,
        out_shape=[jax.ShapeDtypeStruct(local, F32)] * 3,
        name="finish",
    )(sums, precond, *arrays)


def on_device(
    solution,
    residual,
    direction,
    precond,
    inv_spec,
    mixing,
    beams,
    slot_band,
    m_order,
    cycle_order,
    inv_noise,
    pix_mask,
):
    applied, sums = operator(
        direction,
        residual,
        inv_noise,
        pix_mask,
        m_order.reshape(16, 128),
        cycle_order.reshape(8, 128),
        beams,
        precond,
        inv_spec,
        mixing,
        slot_band,
    )
    return tuple(finish(sums, precond, solution, residual, direction, applied))


def solution(mesh):
    finer = Mesh(
        mesh.devices.reshape(mesh.shape["band"], 8, 4, 2), ("band", "blk_0", "blk_1", "blk_2")
    )
    in_specs = (
        P(None, None, BLK, "band"),
        P(None, None, BLK, "band"),
        P(None, None, BLK, "band"),
        P(None, "band"),
        P(None, "band"),
        P(),
        P(),
        P(),
        P(),
        P(),
        P("band", None, BLK, None),
        P(BLK, None),
    )
    out_specs = (P(None, None, BLK, "band"), P(None, None, BLK, "band"), P(None, None, BLK, "band"))
    return jax.shard_map(
        on_device, mesh=finer, in_specs=in_specs, out_specs=out_specs, check_vma=False
    )
```

```python
import math

import jax
import jax.numpy as jnp
from jax import lax
from jax.experimental import pallas as pl
from jax.experimental.pallas import tpu as pltpu
from jax.sharding import Mesh
from jax.sharding import PartitionSpec as P

COMP = 3
STOKES = 3
FIELDS = 9
BANDS = 9
SLOTS = 3
L = 2048
CYCLES = 1024
MODES = 2048
PHI = 4096
QUARTER = PHI // 4
M_DEV = 32
R_DEV = 16
BLOCKS = 64
L_DEV = 512
BLK = ("blk_0", "blk_1", "blk_2")
SCALE = 1.0 / math.sqrt(2048)
VMEM = pltpu.VMEM
MESH = pl.DeviceIdType.MESH
F32 = jnp.float32
BF16 = jnp.bfloat16
NT = (((1,), (1,)), ((), ()))
NN = (((1,), (0,)), ((), ()))


def in_vmem():
    return pl.BlockSpec(memory_space=VMEM)


def in_smem():
    return pl.BlockSpec(memory_space=pltpu.SMEM)


def unit_circle(turn):
    half = (((turn + 2048) & 4095) - 2048).astype(F32) * (math.pi / 4096)
    sq = half * half
    sine = half * (
        1
        + sq
        * (-1 / 6 + sq * (1 / 120 + sq * (-1 / 5040 + sq * (1 / 362880 + sq * (-1 / 39916800)))))
    )
    cosine = 1 + sq * (
        -1 / 2
        + sq
        * (
            1 / 24
            + sq * (-1 / 720 + sq * (1 / 40320 + sq * (-1 / 3628800 + sq * (1 / 479001600))))
        )
    )
    return cosine * cosine - sine * sine, 2 * sine * cosine


def first_turns(mult):
    lane = lax.broadcasted_iota(jnp.int32, mult.shape, 1)
    cosine, sine = unit_circle((mult * lane) & 4095)
    step_cos, step_sin = unit_circle((mult * 128) & 4095)
    return cosine * SCALE, sine * SCALE, step_cos, step_sin


def colat_rows(mult, store):
    cosine, sine, step_cos, step_sin = first_turns(mult)
    for tile in range(L // 128):
        store(tile, cosine.astype(BF16))
        cosine, sine = cosine * step_cos - sine * step_sin, sine * step_cos + cosine * step_sin


def azim_rows(mult, store):
    cosine, sine, step_cos, step_sin = first_turns(mult)
    for tile in range(QUARTER // 128):
        store(tile, cosine.astype(BF16), (-sine).astype(BF16))
        cosine, sine = cosine * step_cos - sine * step_sin, sine * step_cos + cosine * step_sin


STEP = 32


def azim_columns(order, first_turn, store):
    cell = lax.broadcasted_iota(jnp.int32, (STEP, 128), 0)
    cosine, sine = unit_circle((order * cell + first_turn) & 4095)
    step_cos, step_sin = unit_circle((order * STEP) & 4095)
    cosine, sine = cosine * SCALE, sine * SCALE
    for step in range(QUARTER // STEP):
        store(step, cosine.astype(BF16))
        cosine, sine = cosine * step_cos - sine * step_sin, sine * step_cos + cosine * step_sin


def spread(values, row):
    line = values[pl.ds(row, 1), :].astype(F32)
    return jnp.broadcast_to(line, (128, 128)).T.astype(jnp.int32)


def at_least(orders, first):
    l_values = first + lax.broadcasted_iota(jnp.int32, (M_DEV, 256), 1)
    return (l_values >= jnp.concatenate([orders, orders], axis=1)).astype(F32)


def partner(value, low):
    return jnp.where(low, pltpu.roll(value, 96, 1), pltpu.roll(value, 32, 1))


def folded(value):
    tiles = [
        value[8 * i : 8 * i + 8, 128 * j : 128 * j + 128]
        for i in range(value.shape[0] // 8)
        for j in range(value.shape[1] // 128)
    ]
    while len(tiles) > 1:
        tiles = [first + second for first, second in zip(tiles[::2], tiles[1::2])]
    return tiles[0]


def operator_kernel(
    direction_in,
    residual_in,
    noise_in,
    mask_in,
    m_rows,
    cycle_rows,
    beams,
    precond,
    inv_spec,
    mixing,
    slot_band,
    applied,
    sums,
    direction,
    residual,
    noise,
    mask,
    gathered,
    colat,
    azim,
    azim_across,
    turns,
    order_lanes,
    orders,
    beam,
    amps,
    there,
    there_mid,
    arrived,
    turned,
    weighted,
    home,
    home_mid,
    returned,
    flipped,
    combined,
    parts,
    totals,
    sum_y,
    sum_z,
    sum_x,
    load_sem,
    gather_send,
    gather_recv,
    z_send,
    z_recv,
    y_send,
    y_recv,
    x_send,
    x_recv,
    sum_send,
    sum_recv,
):
    x_me = lax.axis_index("band")
    z_me = lax.axis_index("blk_0")
    y_me = lax.axis_index("blk_1") * 2 + lax.axis_index("blk_2")
    right, left, across = (lax.rem(x_me + off, 4) for off in (1, 3, 2))
    z_others = [lax.rem(z_me + off, 8) for off in range(1, 8)]
    y_others = [lax.rem(y_me + off, 8) for off in range(1, 8)]

    def at_x(index):
        return {"band": index}

    def at_z(index):
        return {"blk_0": index}

    def at_y(index):
        return {"blk_1": lax.div(index, 2), "blk_2": lax.rem(index, 2)}

    peers = [at_x(i) for i in (right, left, across)]
    peers += [at_z(i) for i in z_others] + [at_y(i) for i in y_others]
    barrier = pltpu.get_barrier_semaphore()
    for peer in peers:
        pl.semaphore_signal(barrier, inc=1, device_id=peer, device_id_type=MESH)

    loads = [
        pltpu.make_async_copy(source, target, load_sem.at[index])
        for index, (source, target) in enumerate(
            ((direction_in, direction), (mask_in, mask), (noise_in, noise), (residual_in, residual))
        )
    ]
    for load in loads:
        load.start()

    sent = []

    def describe(source, target, send_sem, recv_sem, peer):
        return pltpu.make_async_remote_copy(
            src_ref=source,
            dst_ref=target,
            send_sem=send_sem,
            recv_sem=recv_sem,
            device_id=peer,
            device_id_type=MESH,
        )

    def send(*ends):
        copy = describe(*ends)
        copy.start()
        sent.append(copy)
        return copy

    def arrive(copies):
        for copy in copies:
            copy.wait_recv()

    def halve(s):
        for k in range(2):
            for c in range(COMP):
                gathered[s, x_me, k, c] = direction[c * 3 + s, k].astype(BF16)

    def gather(s):
        return [
            send(
                gathered.at[s, x_me],
                gathered.at[s, x_me],
                gather_send.at[s, way],
                gather_recv.at[s, way],
                at_x(peer),
            )
            for way, peer in enumerate((right, left))
        ]

    def forward_on(s):
        return [
            send(
                gathered.at[s, source, way],
                gathered.at[s, source, way],
                gather_send.at[s, 2 + way],
                gather_recv.at[s, 2 + way],
                at_x(peer),
            )
            for way, (source, peer) in enumerate(((left, right), (right, left)))
        ]

    def make_colat():
        @pl.loop(0, CYCLES // 128)
        def _(block):
            mult = 2 * spread(cycle_rows, block) + 1
            for sub in range(4):
                rows = pl.ds(pl.multiple_of(block * 128 + sub * 32, 32), 32)

                def put(tile, value):
                    colat[rows, tile * 128 : (tile + 1) * 128] = value

                colat_rows(mult[sub * 32 : sub * 32 + 32], put)

    def make_azim(begin, end):
        @pl.loop(begin, end)
        def _(block):
            mult = spread(m_rows, block)
            for sub in range(4):
                first = block * 256 + sub * 64
                real_rows = pl.ds(pl.multiple_of(first, 32), 32)
                imag_rows = pl.ds(pl.multiple_of(first + 32, 32), 32)

                def put(tile, real, imag):
                    azim[real_rows, tile * 128 : (tile + 1) * 128] = real
                    azim[imag_rows, tile * 128 : (tile + 1) * 128] = imag

                azim_rows(mult[sub * 32 : sub * 32 + 32], put)

    def make_azim_across(begin, end):
        @pl.loop(begin, end)
        def _(tile):
            cols = pl.ds(pl.multiple_of(tile * 128, 128), 128)
            order = order_lanes[tile % 2, pl.ds(tile // 2, 1), :]
            part = lax.broadcasted_iota(jnp.int32, (1, 128), 1) & 32

            def put(step, value):
                azim_across[step * STEP : (step + 1) * STEP, cols] = value

            azim_columns(order, part * 32, put)

    mix = [[None] * COMP for _ in range(SLOTS)]
    for x in range(SLOTS):
        slot = slot_band[x_me * SLOTS + x]
        for c in range(COMP):
            mix[x][c] = jnp.where(slot < BANDS, mixing[c, jnp.minimum(slot, BANDS - 1)], 0.0)

    def make_small():
        place = lax.broadcasted_iota(jnp.int32, (16, 128), 1)
        line = m_rows[...]
        even = jnp.where(
            place < 32, line, jnp.where(place < 96, pltpu.roll(line, 32, 1), pltpu.roll(line, 64, 1))
        )
        odd = jnp.where(
            place < 32, pltpu.roll(line, 64, 1), jnp.where(place < 96, pltpu.roll(line, 96, 1), line)
        )
        way = jnp.where((place & 63) < 32, 1.0, -1.0)
        for parity, value in enumerate((even, odd)):
            order_lanes[parity] = value
            phase = value & 3
            turns[0, parity] = jnp.where((value & 1) == 0, 1.0, -1.0)
            turns[1, parity] = jnp.where(phase == 0, 1.0, jnp.where(phase == 2, -1.0, 0.0))
            turns[2, parity] = way * jnp.where(
                phase == 1, 1.0, jnp.where(phase == 3, -1.0, 0.0)
            )
        for x in range(SLOTS):
            slot = slot_band[x_me * SLOTS + x]
            total = jnp.zeros((1, L), F32)
            for band in range(BANDS):
                total = jnp.where(slot == band, beams[band : band + 1, :], total)
            beam[x : x + 1, :] = total
        blk = z_me * 8 + y_me
        all_orders = spread(m_rows, lax.div(blk, 4))
        for sub in range(4):

            @pl.when(lax.rem(blk, 4) == sub)
            def _():
                orders[...] = all_orders[sub * 32 : sub * 32 + 32]

    def turns_of(tile):
        return [turns[index, tile % 2, pl.ds(tile // 2, 1), :] for index in range(3)]

    lane = lax.broadcasted_iota(jnp.int32, (R_DEV, 128), 1)
    on_left = lane < 64
    on_left8 = on_left[:8]
    low = (lane & 63) < 32

    def legendre(s):
        @pl.loop(0, L // 256)
        def _(block):
            first = pl.multiple_of(block * 256, 256)
            piece = block // 2
            inner = pl.ds(pl.multiple_of((block % 2) * 256, 256), 256)
            triangle = at_least(orders[...], first)
            for k in range(2):
                comps = [gathered[s, piece, k, c, :, inner].astype(F32) for c in range(COMP)]
                for x in range(SLOTS):
                    mixed = mix[x][0] * comps[0]
                    for c in range(1, COMP):
                        mixed = mixed + mix[x][c] * comps[c]
                    row = (x * 2 + k) * M_DEV
                    value = mixed * beam[x : x + 1, pl.ds(first, 256)] * triangle
                    amps[row : row + M_DEV, pl.ds(first, 256)] = value.astype(BF16)

        @pl.loop(0, CYCLES // 256)
        def _(block):
            rows = pl.ds(pl.multiple_of(block * 256, 256), 256)
            side = lax.dot_general(colat[rows, :], amps[...], NT, preferred_element_type=F32)
            main = side[:, :128].reshape(2, 8, 16, 128)
            tail = side[:, 128:].reshape(16, 16, 128)
            wide = lax.broadcasted_iota(jnp.int32, (128, 128), 1) < 64
            packed = jnp.where(
                wide,
                tail[:, :8].reshape(128, 128),
                pltpu.roll(tail[:, 8:].reshape(128, 128), 64, 1),
            )
            there[s, pl.ds(block * 2, 2), :, 0:16, :] = main.astype(BF16)
            there[s, pl.ds(block * 2, 2), :, 16:24, :] = packed.reshape(2, 8, 8, 128).astype(BF16)

    def z_copy(way, s, off, source, middle):
        other = lax.rem(z_me + off, 8)
        return describe(
            source.at[s, other],
            middle.at[s, z_me],
            z_send.at[way, s, off - 1],
            z_recv.at[way, s, off - 1],
            at_z(other),
        )

    def start_z(way, s, source, middle):
        for off in (1, 7, 2, 6, 3, 5, 4):
            z_copy(way, s, off, source, middle).start()

    def y_copy(way, s, index, source, target):
        return describe(
            source, target, y_send.at[way, s, index], y_recv.at[way, s, index], at_y(y_others[index])
        )

    def pass_on(way, s, source, middle, target):
        for off in (0, 1, 7, 2, 6, 3, 5, 4):
            plane = lax.rem(z_me + 8 - off, 8)
            held = source if off == 0 else middle
            if off:
                copy = z_copy(way, s, off, source, middle)
                copy.wait_recv()
                sent.append(copy)
            for index, other in enumerate(y_others):
                y_copy(
                    way, s, index, held.at[s, plane, other], target.at[s, plane, y_me]
                ).start()
            target[s, plane, y_me] = held[s, plane, y_me]

    def wait_y(way, s, middle, target):
        for index, other in enumerate(y_others):
            copy = y_copy(way, s, index, middle.at[s, :, other], target.at[s, :, y_me])
            copy.wait_recv()
            sent.append(copy)

    def azimuth(s, between):
        @pl.loop(0, BLOCKS // 2, unroll=4)
        def _(tile):
            cols = pl.ds(pl.multiple_of(tile * 128, 128), 128)
            sign, cosine, sine = turns_of(tile)
            plane, place = tile // 4, (tile % 4) * 2
            first = arrived[s, plane, place, 0:16, :].astype(F32)
            second = arrived[s, plane, place + 1, 0:16, :].astype(F32)
            third = arrived[s, plane, place, 16:24, :].astype(F32)
            fourth = arrived[s, plane, place + 1, 16:24, :].astype(F32)
            values = [
                jnp.where(on_left, first, pltpu.roll(second, 64, 1)),
                jnp.where(on_left, pltpu.roll(first, 64, 1), second),
                jnp.concatenate(
                    [
                        jnp.where(on_left8, third, pltpu.roll(fourth, 64, 1)),
                        jnp.where(on_left8, pltpu.roll(third, 64, 1), fourth),
                    ],
                    axis=0,
                ),
            ]
            for x, value in enumerate(values):
                straight = cosine * value
                crossed = sine * partner(value, low)
                for q, part in enumerate(
                    (value, straight - crossed, sign * value, straight + crossed)
                ):
                    row = q * 48 + x * R_DEV
                    turned[row : row + R_DEV, cols] = part.astype(BF16)

        @pl.loop(0, QUARTER // 256, unroll=2)
        def _(block):
            start = pl.multiple_of(block * 256, 256)
            cols = pl.ds(start, 256)
            sky = lax.dot_general(turned[...], azim[:, cols], NN, preferred_element_type=F32)
            for q in range(4):
                cells = pl.ds(pl.multiple_of(q * QUARTER + start, 256), 256)
                keep = mask[:, cells].astype(F32)
                for x in range(SLOTS):
                    row = q * 48 + x * R_DEV
                    weight = noise[x, s, :, cells] * keep
                    weighted[row : row + R_DEV, cols] = (
                        weight * sky[row : row + R_DEV, :]
                    ).astype(BF16)

        between()

        @pl.loop(1, 9)
        def _(off):
            home_plane = lax.rem(z_me + off, 8)
            backs = []
            for half in range(2):
                cols = pl.ds(pl.multiple_of(home_plane * 512 + half * 256, 256), 256)
                backs.append(
                    lax.dot_general(
                        weighted[...], azim_across[:, cols], NN, preferred_element_type=F32
                    )
                )
            for inner in range(4):
                tile = home_plane * 4 + inner
                back, sub = backs[inner // 2], inner % 2
                sign, cosine, sine = turns_of(tile)
                lanes = slice(sub * 128, sub * 128 + 128)
                values = []
                for x in range(SLOTS):
                    b0, b1, b2, b3 = (
                        back[q * 48 + x * R_DEV : q * 48 + x * R_DEV + R_DEV, lanes]
                        for q in range(4)
                    )
                    values.append(
                        b0 + sign * b2 + cosine * (b1 + b3) + sine * partner(b1 - b3, low)
                    )
                zero, one, two = values
                plane, place = home_plane, inner * 2
                home[s, plane, place, 0:16, :] = jnp.where(
                    on_left, zero, pltpu.roll(one, 64, 1)
                ).astype(BF16)
                home[s, plane, place + 1, 0:16, :] = jnp.where(
                    on_left, pltpu.roll(zero, 64, 1), one
                ).astype(BF16)
                home[s, plane, place, 16:24, :] = jnp.where(
                    on_left8, two[:8], pltpu.roll(two[8:], 64, 1)
                ).astype(BF16)
                home[s, plane, place + 1, 16:24, :] = jnp.where(
                    on_left8, pltpu.roll(two[:8], 64, 1), two[8:]
                ).astype(BF16)

            @pl.when(off < 8)
            def _():
                z_copy(1, s, off, home, home_mid).start()

    def legendre_back(s):
        @pl.loop(0, 8)
        def _(plane):
            cols = pl.ds(pl.multiple_of(plane * 128, 128), 128)
            main = returned[s, plane, :, 0:16, :].astype(F32).reshape(128, 128)
            tail = returned[s, plane, :, 16:24, :].astype(F32)
            swapped = pltpu.roll(tail.reshape(64, 128), 64, 1).reshape(8, 8, 128)
            both = jnp.concatenate([tail, swapped], axis=1).reshape(128, 128)
            flipped[0:128, cols] = main.T.astype(BF16)
            flipped[128:256, cols] = both.T.astype(BF16)

        @pl.loop(1, 5)
        def _(off):
            piece = lax.rem(x_me + off, 4)
            for half in range(2):
                start = pl.multiple_of(piece * L_DEV + half * 256, 256)
                harm = lax.dot_general(
                    flipped[0:192, :],
                    colat[:, pl.ds(start, 256)],
                    NN,
                    preferred_element_type=F32,
                )
                triangle = at_least(orders[...], start)
                inner = slice(half * 256, half * 256 + 256)
                for k in range(2):
                    shaped = []
                    for x in range(SLOTS):
                        row = (x * 2 + k) * M_DEV
                        shaped.append(
                            harm[row : row + M_DEV, :]
                            * beam[x : x + 1, pl.ds(start, 256)]
                            * triangle
                        )
                    for c in range(COMP):
                        total = mix[0][c] * shaped[0]
                        for x in range(1, SLOTS):
                            total = total + mix[x][c] * shaped[x]
                        combined[s, piece, c, k, :, inner] = total.astype(BF16)

            @pl.when(off < 4)
            def _():
                x_copy(s, off).start()

    def x_copy(s, off):
        other = lax.rem(x_me + off, 4)
        return describe(
            combined.at[s, other],
            parts.at[s, off - 1],
            x_send.at[s, off - 1],
            x_recv.at[s, off - 1],
            at_x(other),
        )

    def wait_x(s):
        for off in range(1, 4):
            copy = x_copy(s, off)
            copy.wait_recv()
            sent.append(copy)

    def apply(s):
        for c in range(COMP):
            field = c * 3 + s
            pre = precond[field : field + 1, :]
            prior = inv_spec[field : field + 1, :]
            for k in range(2):
                total = combined[s, x_me, c, k].astype(F32)
                for index in range(3):
                    total = total + parts[s, index, c, k].astype(F32)
                dir_now = direction[field, k]
                res_now = residual[field, k]
                value = prior * dir_now + total
                applied[field, k] = value
                scaled = pre * res_now
                totals[0] += folded(res_now * scaled)
                totals[1] += folded(dir_now * value)
                totals[2] += folded(value * scaled)
                totals[3] += folded(value * pre * value)

    def sum_over(stage, buffer, me, others, place, value):
        buffer[me] = value
        copies = [
            send(
                buffer.at[me],
                buffer.at[me],
                sum_send.at[stage, index],
                sum_recv.at[stage, index],
                place(other),
            )
            for index, other in enumerate(others)
        ]
        arrive(copies)
        return jnp.sum(buffer[...], axis=0)

    loads[0].wait()
    halve(0)
    pl.semaphore_wait(barrier, len(peers))
    direct = gather(0)
    halve(1)
    halve(2)
    totals[...] = jnp.zeros_like(totals)
    amps[192:256, :] = jnp.zeros((64, L), BF16)
    make_small()
    make_colat()
    arrive(direct)
    relayed = forward_on(0)
    direct = gather(1)
    make_azim(0, 8)
    arrive(relayed)
    legendre(0)
    start_z(0, 0, there, there_mid)
    arrive(direct)
    relayed = forward_on(1)
    direct = gather(2)
    make_azim(8, 16)
    arrive(relayed)
    legendre(1)
    start_z(0, 1, there, there_mid)
    arrive(direct)
    relayed = forward_on(2)
    make_azim_across(0, 16)
    pass_on(0, 0, there, there_mid, arrived)
    arrive(relayed)
    legendre(2)
    start_z(0, 2, there, there_mid)
    make_azim_across(16, 32)
    for load in loads[1:]:
        load.wait()
    wait_y(0, 0, there_mid, arrived)
    azimuth(0, lambda: pass_on(0, 1, there, there_mid, arrived))
    wait_y(0, 1, there_mid, arrived)
    azimuth(1, lambda: pass_on(0, 2, there, there_mid, arrived))
    pass_on(1, 0, home, home_mid, returned)
    wait_y(0, 2, there_mid, arrived)

    def first_back():
        wait_y(1, 0, home_mid, returned)
        legendre_back(0)

    azimuth(2, first_back)
    pass_on(1, 1, home, home_mid, returned)
    wait_y(1, 1, home_mid, returned)
    legendre_back(1)
    pass_on(1, 2, home, home_mid, returned)
    wait_x(0)
    apply(0)
    wait_y(1, 2, home_mid, returned)
    legendre_back(2)
    wait_x(1)
    apply(1)
    wait_x(2)
    apply(2)

    row = lax.broadcasted_iota(jnp.int32, (8, 128), 0)
    value = jnp.zeros((8, 128), F32)
    for index in range(4):
        value = jnp.where(row == index, jnp.sum(totals[index], axis=0, keepdims=True), value)
    value = sum_over(0, sum_y, y_me, y_others, at_y, value)
    value = sum_over(1, sum_z, z_me, z_others, at_z, value)
    value = sum_over(2, sum_x, x_me, (right, left, across), at_x, value)
    sums[...] = jnp.broadcast_to(jnp.sum(value, axis=1, keepdims=True), (8, 128))
    for copy in sent:
        copy.wait_send()


def operator(direction, residual, noise, mask, *small):
    dma = pltpu.SemaphoreType.DMA
    block = (STOKES, 8, 8, 24, 128)
    local = (FIELDS, 2, M_DEV, L_DEV)
    return pl.pallas_call(
        operator_kernel,
        in_specs=[pl.BlockSpec(memory_space=pl.ANY)] * 4 + [in_vmem()] * 5 + [in_smem()] * 2,
        out_specs=[in_vmem(), in_vmem()],
        out_shape=[jax.ShapeDtypeStruct(local, F32), jax.ShapeDtypeStruct((8, 128), F32)],
        scratch_shapes=[
            VMEM(local, F32),
            VMEM(local, F32),
            VMEM((SLOTS, STOKES, R_DEV, PHI), F32),
            VMEM((R_DEV, PHI), jnp.int32),
            VMEM((STOKES, 4, 2, COMP, M_DEV, L_DEV), BF16),
            VMEM((CYCLES, L), BF16),
            VMEM((2 * MODES, QUARTER), BF16),
            VMEM((QUARTER, 2 * MODES), BF16),
            VMEM((3, 2, 16, 128), F32),
            VMEM((2, 16, 128), jnp.int32),
            VMEM((M_DEV, 128), jnp.int32),
            VMEM((SLOTS, L), F32),
            VMEM((256, L), BF16),
            VMEM(block, BF16),
            VMEM(block, BF16),
            VMEM(block, BF16),
            VMEM((192, 2 * MODES), BF16),
            VMEM((192, QUARTER), BF16),
            VMEM(block, BF16),
            VMEM(block, BF16),
            VMEM(block, BF16),
            VMEM((256, CYCLES), BF16),
            VMEM((STOKES, 4, COMP, 2, M_DEV, L_DEV), BF16),
            VMEM((STOKES, 3, COMP, 2, M_DEV, L_DEV), BF16),
            VMEM((4, 8, 128), F32),
            VMEM((8, 8, 128), F32),
            VMEM((8, 8, 128), F32),
            VMEM((4, 8, 128), F32),
            dma((4,)),
            dma((STOKES, 4)),
            dma((STOKES, 4)),
            dma((2, STOKES, 7)),
            dma((2, STOKES, 7)),
            dma((2, STOKES, 7)),
            dma((2, STOKES, 7)),
            dma((STOKES, 3)),
            dma((STOKES, 3)),
            dma((3, 7)),
            dma((3, 7)),
        ],
        compiler_params=pltpu.CompilerParams(
            collective_id=0, has_side_effects=True, vmem_limit_bytes=60 * 1024 * 1024
        ),
        name="operator",
    )(direction, residual, noise, mask, *small)


def finish_kernel(sums, precond, solution, residual, direction, applied, out_sol, out_res, out_dir):
    norm_old, curvature, crossed, squared = (
        jnp.concatenate([sums[index : index + 1, :]] * 4, axis=1) for index in range(4)
    )
    step_size = norm_old / curvature
    norm_new = norm_old - 2.0 * step_size * crossed + step_size * step_size * squared
    ratio = norm_new / norm_old
    for field in range(COMP):
        pre = precond[pl.ds(pl.program_id(0) * COMP + field, 1), :]
        for k in range(2):
            dir_now = direction[field, k]
            res_next = residual[field, k] - step_size * applied[field, k]
            out_sol[field, k] = solution[field, k] + step_size * dir_now
            out_res[field, k] = res_next
            out_dir[field, k] = pre * res_next + ratio * dir_now


def finish(sums, precond, *arrays):
    local = (FIELDS, 2, M_DEV, L_DEV)
    field = pl.BlockSpec((COMP, 2, M_DEV, L_DEV), lambda g: (g, 0, 0, 0))
    whole = [pl.BlockSpec((8, 128), lambda g: (0, 0)), pl.BlockSpec((FIELDS, L_DEV), lambda g: (0, 0))]
    return pl.pallas_call(
        finish_kernel,
        grid=(FIELDS // COMP,),
        in_specs=whole + [field] * 4,
        out_specs=[field] * 3,
        out_shape=[jax.ShapeDtypeStruct(local, F32)] * 3,
        name="finish",
    )(sums, precond, *arrays)


def on_device(
    solution,
    residual,
    direction,
    precond,
    inv_spec,
    mixing,
    beams,
    slot_band,
    m_order,
    cycle_order,
    inv_noise,
    pix_mask,
):
    applied, sums = operator(
        direction,
        residual,
        inv_noise,
        pix_mask,
        m_order.reshape(16, 128),
        cycle_order.reshape(8, 128),
        beams,
        precond,
        inv_spec,
        mixing.T,
        slot_band,
    )
    return tuple(finish(sums, precond, solution, residual, direction, applied))


def solution(mesh):
    finer = Mesh(
        mesh.devices.reshape(mesh.shape["band"], 8, 4, 2), ("band", "blk_0", "blk_1", "blk_2")
    )
    in_specs = (
        P(None, None, BLK, "band"),
        P(None, None, BLK, "band"),
        P(None, None, BLK, "band"),
        P(None, "band"),
        P(None, "band"),
        P(),
        P(),
        P(),
        P(),
        P(),
        P("band", None, BLK, None),
        P(BLK, None),
    )
    out_specs = (P(None, None, BLK, "band"), P(None, None, BLK, "band"), P(None, None, BLK, "band"))
    return jax.shard_map(
        on_device, mesh=finer, in_specs=in_specs, out_specs=out_specs, check_vma=False
    )
```

```python
import math

import jax
import jax.numpy as jnp
from jax import lax
from jax.experimental import pallas as pl
from jax.experimental.pallas import tpu as pltpu
from jax.sharding import Mesh
from jax.sharding import PartitionSpec as P

COMP = 3
STOKES = 3
FIELDS = 9
BANDS = 9
SLOTS = 3
L = 2048
CYCLES = 1024
MODES = 2048
PHI = 4096
QUARTER = PHI // 4
M_DEV = 32
R_DEV = 16
BLOCKS = 64
L_DEV = 512
BLK = ("blk_0", "blk_1", "blk_2")
SCALE = 1.0 / math.sqrt(2048)
VMEM = pltpu.VMEM
MESH = pl.DeviceIdType.MESH
F32 = jnp.float32
BF16 = jnp.bfloat16
NT = (((1,), (1,)), ((), ()))
NN = (((1,), (0,)), ((), ()))


def in_vmem():
    return pl.BlockSpec(memory_space=VMEM)


def in_smem():
    return pl.BlockSpec(memory_space=pltpu.SMEM)


def unit_circle(turn):
    half = (((turn + 2048) & 4095) - 2048).astype(F32) * (math.pi / 4096)
    sq = half * half
    sine = half * (
        1
        + sq
        * (-1 / 6 + sq * (1 / 120 + sq * (-1 / 5040 + sq * (1 / 362880 + sq * (-1 / 39916800)))))
    )
    cosine = 1 + sq * (
        -1 / 2
        + sq
        * (
            1 / 24
            + sq * (-1 / 720 + sq * (1 / 40320 + sq * (-1 / 3628800 + sq * (1 / 479001600))))
        )
    )
    return cosine * cosine - sine * sine, 2 * sine * cosine


def first_turns(mult):
    lane = lax.broadcasted_iota(jnp.int32, mult.shape, 1)
    cosine, sine = unit_circle((mult * lane) & 4095)
    step_cos, step_sin = unit_circle((mult * 128) & 4095)
    return cosine * SCALE, sine * SCALE, step_cos, step_sin


def colat_rows(mult, store):
    cosine, sine, step_cos, step_sin = first_turns(mult)
    for tile in range(L // 128):
        store(tile, cosine.astype(BF16))
        cosine, sine = cosine * step_cos - sine * step_sin, sine * step_cos + cosine * step_sin


def azim_rows(mult, store):
    cosine, sine, step_cos, step_sin = first_turns(mult)
    for tile in range(QUARTER // 128):
        store(tile, cosine.astype(BF16), (-sine).astype(BF16))
        cosine, sine = cosine * step_cos - sine * step_sin, sine * step_cos + cosine * step_sin


STEP = 32


def azim_columns(order, first_turn, store):
    cell = lax.broadcasted_iota(jnp.int32, (STEP, 128), 0)
    cosine, sine = unit_circle((order * cell + first_turn) & 4095)
    step_cos, step_sin = unit_circle((order * STEP) & 4095)
    cosine, sine = cosine * SCALE, sine * SCALE
    for step in range(QUARTER // STEP):
        store(step, cosine.astype(BF16))
        cosine, sine = cosine * step_cos - sine * step_sin, sine * step_cos + cosine * step_sin


def spread(values, row):
    line = values[pl.ds(row, 1), :].astype(F32)
    return jnp.broadcast_to(line, (128, 128)).T.astype(jnp.int32)


def at_least(orders, first):
    l_values = first + lax.broadcasted_iota(jnp.int32, (M_DEV, 256), 1)
    return (l_values >= jnp.concatenate([orders, orders], axis=1)).astype(F32)


def partner(value, low):
    return jnp.where(low, pltpu.roll(value, 96, 1), pltpu.roll(value, 32, 1))


def folded(value):
    tiles = [
        value[8 * i : 8 * i + 8, 128 * j : 128 * j + 128]
        for i in range(value.shape[0] // 8)
        for j in range(value.shape[1] // 128)
    ]
    while len(tiles) > 1:
        tiles = [first + second for first, second in zip(tiles[::2], tiles[1::2])]
    return tiles[0]


def operator_kernel(
    direction_in,
    residual_in,
    noise_in,
    mask_in,
    m_rows,
    cycle_rows,
    beams,
    precond,
    inv_spec,
    mixing,
    slot_band,
    applied,
    sums,
    direction,
    residual,
    noise,
    mask,
    gathered,
    colat,
    azim,
    azim_across,
    turns,
    order_lanes,
    orders,
    beam,
    amps,
    there,
    there_mid,
    arrived,
    turned,
    weighted,
    home,
    home_mid,
    returned,
    flipped,
    combined,
    parts,
    totals,
    sum_y,
    sum_z,
    sum_x,
    load_sem,
    gather_send,
    gather_recv,
    z_send,
    z_recv,
    y_send,
    y_recv,
    x_send,
    x_recv,
    sum_send,
    sum_recv,
):
    x_me = lax.axis_index("band")
    z_me = lax.axis_index("blk_0")
    y_me = lax.axis_index("blk_1") * 2 + lax.axis_index("blk_2")
    right, left, across = (lax.rem(x_me + off, 4) for off in (1, 3, 2))
    z_others = [lax.rem(z_me + off, 8) for off in range(1, 8)]
    y_others = [lax.rem(y_me + off, 8) for off in range(1, 8)]

    def at_x(index):
        return {"band": index}

    def at_z(index):
        return {"blk_0": index}

    def at_y(index):
        return {"blk_1": lax.div(index, 2), "blk_2": lax.rem(index, 2)}

    peers = [at_x(i) for i in (right, left, across)]
    peers += [at_z(i) for i in z_others] + [at_y(i) for i in y_others]
    barrier = pltpu.get_barrier_semaphore()
    for peer in peers:
        pl.semaphore_signal(barrier, inc=1, device_id=peer, device_id_type=MESH)

    loads = [
        pltpu.make_async_copy(source, target, load_sem.at[index])
        for index, (source, target) in enumerate(
            ((direction_in, direction), (mask_in, mask), (noise_in, noise), (residual_in, residual))
        )
    ]
    for load in loads:
        load.start()

    sent = []

    def describe(source, target, send_sem, recv_sem, peer):
        return pltpu.make_async_remote_copy(
            src_ref=source,
            dst_ref=target,
            send_sem=send_sem,
            recv_sem=recv_sem,
            device_id=peer,
            device_id_type=MESH,
        )

    def send(*ends):
        copy = describe(*ends)
        copy.start()
        sent.append(copy)
        return copy

    def arrive(copies):
        for copy in copies:
            copy.wait_recv()

    def halve(s):
        for k in range(2):
            for c in range(COMP):
                gathered[s, x_me, k, c] = direction[c * 3 + s, k].astype(BF16)

    def gather(s):
        return [
            send(
                gathered.at[s, x_me],
                gathered.at[s, x_me],
                gather_send.at[s, way],
                gather_recv.at[s, way],
                at_x(peer),
            )
            for way, peer in enumerate((right, left))
        ]

    def forward_on(s):
        return [
            send(
                gathered.at[s, source, way],
                gathered.at[s, source, way],
                gather_send.at[s, 2 + way],
                gather_recv.at[s, 2 + way],
                at_x(peer),
            )
            for way, (source, peer) in enumerate(((left, right), (right, left)))
        ]

    def make_colat():
        @pl.loop(0, CYCLES // 128)
        def _(block):
            mult = 2 * spread(cycle_rows, block) + 1
            for sub in range(4):
                rows = pl.ds(pl.multiple_of(block * 128 + sub * 32, 32), 32)

                def put(tile, value):
                    colat[rows, tile * 128 : (tile + 1) * 128] = value

                colat_rows(mult[sub * 32 : sub * 32 + 32], put)

    def make_azim(begin, end):
        @pl.loop(begin, end)
        def _(block):
            mult = spread(m_rows, block)
            for sub in range(4):
                first = block * 256 + sub * 64
                real_rows = pl.ds(pl.multiple_of(first, 32), 32)
                imag_rows = pl.ds(pl.multiple_of(first + 32, 32), 32)

                def put(tile, real, imag):
                    azim[real_rows, tile * 128 : (tile + 1) * 128] = real
                    azim[imag_rows, tile * 128 : (tile + 1) * 128] = imag

                azim_rows(mult[sub * 32 : sub * 32 + 32], put)

    def make_azim_across(begin, end):
        @pl.loop(begin, end)
        def _(tile):
            cols = pl.ds(pl.multiple_of(tile * 128, 128), 128)
            order = order_lanes[tile % 2, pl.ds(tile // 2, 1), :]
            part = lax.broadcasted_iota(jnp.int32, (1, 128), 1) & 32

            def put(step, value):
                azim_across[step * STEP : (step + 1) * STEP, cols] = value

            azim_columns(order, part * 32, put)

    mix = [[None] * COMP for _ in range(SLOTS)]
    for x in range(SLOTS):
        slot = slot_band[x_me * SLOTS + x]
        for c in range(COMP):
            mix[x][c] = jnp.where(slot < BANDS, mixing[c, jnp.minimum(slot, BANDS - 1)], 0.0)

    def make_small():
        place = lax.broadcasted_iota(jnp.int32, (16, 128), 1)
        line = m_rows[...]
        even = jnp.where(
            place < 32, line, jnp.where(place < 96, pltpu.roll(line, 32, 1), pltpu.roll(line, 64, 1))
        )
        odd = jnp.where(
            place < 32, pltpu.roll(line, 64, 1), jnp.where(place < 96, pltpu.roll(line, 96, 1), line)
        )
        way = jnp.where((place & 63) < 32, 1.0, -1.0)
        for parity, value in enumerate((even, odd)):
            order_lanes[parity] = value
            phase = value & 3
            turns[0, parity] = jnp.where((value & 1) == 0, 1.0, -1.0)
            turns[1, parity] = jnp.where(phase == 0, 1.0, jnp.where(phase == 2, -1.0, 0.0))
            turns[2, parity] = way * jnp.where(
                phase == 1, 1.0, jnp.where(phase == 3, -1.0, 0.0)
            )
        for x in range(SLOTS):
            slot = slot_band[x_me * SLOTS + x]
            total = jnp.zeros((1, L), F32)
            for band in range(BANDS):
                total = jnp.where(slot == band, beams[band : band + 1, :], total)
            beam[x : x + 1, :] = total
        blk = z_me * 8 + y_me
        all_orders = spread(m_rows, lax.div(blk, 4))
        for sub in range(4):

            @pl.when(lax.rem(blk, 4) == sub)
            def _():
                orders[...] = all_orders[sub * 32 : sub * 32 + 32]

    def turns_of(tile):
        return [turns[index, tile % 2, pl.ds(tile // 2, 1), :] for index in range(3)]

    lane = lax.broadcasted_iota(jnp.int32, (R_DEV, 128), 1)
    on_left = lane < 64
    on_left8 = on_left[:8]
    low = (lane & 63) < 32

    def legendre(s):
        @pl.loop(0, L // 256)
        def _(block):
            first = pl.multiple_of(block * 256, 256)
            piece = block // 2
            inner = pl.ds(pl.multiple_of((block % 2) * 256, 256), 256)
            triangle = at_least(orders[...], first)
            for k in range(2):
                comps = [gathered[s, piece, k, c, :, inner].astype(F32) for c in range(COMP)]
                for x in range(SLOTS):
                    mixed = mix[x][0] * comps[0]
                    for c in range(1, COMP):
                        mixed = mixed + mix[x][c] * comps[c]
                    row = (x * 2 + k) * M_DEV
                    value = mixed * beam[x : x + 1, pl.ds(first, 256)] * triangle
                    amps[row : row + M_DEV, pl.ds(first, 256)] = value.astype(BF16)

        @pl.loop(0, CYCLES // 256)
        def _(block):
            rows = pl.ds(pl.multiple_of(block * 256, 256), 256)
            side = lax.dot_general(colat[rows, :], amps[...], NT, preferred_element_type=F32)
            main = side[:, :128].reshape(2, 8, 16, 128)
            tail = side[:, 128:].reshape(16, 16, 128)
            wide = lax.broadcasted_iota(jnp.int32, (128, 128), 1) < 64
            packed = jnp.where(
                wide,
                tail[:, :8].reshape(128, 128),
                pltpu.roll(tail[:, 8:].reshape(128, 128), 64, 1),
            )
            there[s, pl.ds(block * 2, 2), :, 0:16, :] = main.astype(BF16)
            there[s, pl.ds(block * 2, 2), :, 16:24, :] = packed.reshape(2, 8, 8, 128).astype(BF16)

    def z_copy(way, s, off, source, middle):
        other = lax.rem(z_me + off, 8)
        return describe(
            source.at[s, other],
            middle.at[s, z_me],
            z_send.at[way, s, off - 1],
            z_recv.at[way, s, off - 1],
            at_z(other),
        )

    def start_z(way, s, source, middle):
        for off in (1, 7, 2, 6, 3, 5, 4):
            z_copy(way, s, off, source, middle).start()

    def y_copy(way, s, index, source, target):
        return describe(
            source, target, y_send.at[way, s, index], y_recv.at[way, s, index], at_y(y_others[index])
        )

    def pass_on(way, s, source, middle, target):
        for off in (0, 1, 7, 2, 6, 3, 5, 4):
            plane = lax.rem(z_me + 8 - off, 8)
            held = source if off == 0 else middle
            if off:
                copy = z_copy(way, s, off, source, middle)
                copy.wait_recv()
                sent.append(copy)
            for index, other in enumerate(y_others):
                y_copy(
                    way, s, index, held.at[s, plane, other], target.at[s, plane, y_me]
                ).start()
            target[s, plane, y_me] = held[s, plane, y_me]

    def wait_y(way, s, middle, target):
        for index, other in enumerate(y_others):
            copy = y_copy(way, s, index, middle.at[s, :, other], target.at[s, :, y_me])
            copy.wait_recv()
            sent.append(copy)

    def azimuth(s, between):
        @pl.loop(0, BLOCKS // 2, unroll=4)
        def _(tile):
            cols = pl.ds(pl.multiple_of(tile * 128, 128), 128)
            sign, cosine, sine = turns_of(tile)
            plane, place = tile // 4, (tile % 4) * 2
            first = arrived[s, plane, place, 0:16, :].astype(F32)
            second = arrived[s, plane, place + 1, 0:16, :].astype(F32)
            third = arrived[s, plane, place, 16:24, :].astype(F32)
            fourth = arrived[s, plane, place + 1, 16:24, :].astype(F32)
            values = [
                jnp.where(on_left, first, pltpu.roll(second, 64, 1)),
                jnp.where(on_left, pltpu.roll(first, 64, 1), second),
                jnp.concatenate(
                    [
                        jnp.where(on_left8, third, pltpu.roll(fourth, 64, 1)),
                        jnp.where(on_left8, pltpu.roll(third, 64, 1), fourth),
                    ],
                    axis=0,
                ),
            ]
            for x, value in enumerate(values):
                straight = cosine * value
                crossed = sine * partner(value, low)
                for q, part in enumerate(
                    (value, straight - crossed, sign * value, straight + crossed)
                ):
                    row = q * 48 + x * R_DEV
                    turned[row : row + R_DEV, cols] = part.astype(BF16)

        @pl.loop(0, QUARTER // 256, unroll=2)
        def _(block):
            start = pl.multiple_of(block * 256, 256)
            cols = pl.ds(start, 256)
            sky = lax.dot_general(turned[...], azim[:, cols], NN, preferred_element_type=F32)
            for q in range(4):
                cells = pl.ds(pl.multiple_of(q * QUARTER + start, 256), 256)
                keep = mask[:, cells].astype(F32)
                for x in range(SLOTS):
                    row = q * 48 + x * R_DEV
                    weight = noise[x, s, :, cells] * keep
                    weighted[row : row + R_DEV, cols] = (
                        weight * sky[row : row + R_DEV, :]
                    ).astype(BF16)

        between()

        @pl.loop(1, 9)
        def _(off):
            home_plane = lax.rem(z_me + off, 8)
            backs = []
            for half in range(2):
                cols = pl.ds(pl.multiple_of(home_plane * 512 + half * 256, 256), 256)
                backs.append(
                    lax.dot_general(
                        weighted[...], azim_across[:, cols], NN, preferred_element_type=F32
                    )
                )
            for inner in range(4):
                tile = home_plane * 4 + inner
                back, sub = backs[inner // 2], inner % 2
                sign, cosine, sine = turns_of(tile)
                lanes = slice(sub * 128, sub * 128 + 128)
                values = []
                for x in range(SLOTS):
                    b0, b1, b2, b3 = (
                        back[q * 48 + x * R_DEV : q * 48 + x * R_DEV + R_DEV, lanes]
                        for q in range(4)
                    )
                    values.append(
                        b0 + sign * b2 + cosine * (b1 + b3) + sine * partner(b1 - b3, low)
                    )
                zero, one, two = values
                plane, place = home_plane, inner * 2
                home[s, plane, place, 0:16, :] = jnp.where(
                    on_left, zero, pltpu.roll(one, 64, 1)
                ).astype(BF16)
                home[s, plane, place + 1, 0:16, :] = jnp.where(
                    on_left, pltpu.roll(zero, 64, 1), one
                ).astype(BF16)
                home[s, plane, place, 16:24, :] = jnp.where(
                    on_left8, two[:8], pltpu.roll(two[8:], 64, 1)
                ).astype(BF16)
                home[s, plane, place + 1, 16:24, :] = jnp.where(
                    on_left8, pltpu.roll(two[:8], 64, 1), two[8:]
                ).astype(BF16)

            @pl.when(off < 8)
            def _():
                z_copy(1, s, off, home, home_mid).start()

    def legendre_back(s):
        @pl.loop(0, 8)
        def _(plane):
            cols = pl.ds(pl.multiple_of(plane * 128, 128), 128)
            main = returned[s, plane, :, 0:16, :].astype(F32).reshape(128, 128)
            tail = returned[s, plane, :, 16:24, :].astype(F32)
            swapped = pltpu.roll(tail.reshape(64, 128), 64, 1).reshape(8, 8, 128)
            both = jnp.concatenate([tail, swapped], axis=1).reshape(128, 128)
            flipped[0:128, cols] = main.T.astype(BF16)
            flipped[128:256, cols] = both.T.astype(BF16)

        @pl.loop(1, 5)
        def _(off):
            piece = lax.rem(x_me + off, 4)
            for half in range(2):
                start = pl.multiple_of(piece * L_DEV + half * 256, 256)
                harm = lax.dot_general(
                    flipped[0:192, :],
                    colat[:, pl.ds(start, 256)],
                    NN,
                    preferred_element_type=F32,
                )
                triangle = at_least(orders[...], start)
                inner = slice(half * 256, half * 256 + 256)
                for k in range(2):
                    shaped = []
                    for x in range(SLOTS):
                        row = (x * 2 + k) * M_DEV
                        shaped.append(
                            harm[row : row + M_DEV, :]
                            * beam[x : x + 1, pl.ds(start, 256)]
                            * triangle
                        )
                    for c in range(COMP):
                        total = mix[0][c] * shaped[0]
                        for x in range(1, SLOTS):
                            total = total + mix[x][c] * shaped[x]
                        combined[s, piece, c, k, :, inner] = total.astype(BF16)

            @pl.when(off < 4)
            def _():
                x_copy(s, off).start()

    def x_copy(s, off):
        other = lax.rem(x_me + off, 4)
        return describe(
            combined.at[s, other],
            parts.at[s, off - 1],
            x_send.at[s, off - 1],
            x_recv.at[s, off - 1],
            at_x(other),
        )

    def wait_x(s):
        for off in range(1, 4):
            copy = x_copy(s, off)
            copy.wait_recv()
            sent.append(copy)

    def apply(s):
        for c in range(COMP):
            field = c * 3 + s
            pre = precond[field : field + 1, :]
            prior = inv_spec[field : field + 1, :]
            for k in range(2):
                total = combined[s, x_me, c, k].astype(F32)
                for index in range(3):
                    total = total + parts[s, index, c, k].astype(F32)
                dir_now = direction[field, k]
                res_now = residual[field, k]
                value = prior * dir_now + total
                applied[field, k] = value
                scaled = pre * res_now
                totals[0] += folded(res_now * scaled)
                totals[1] += folded(dir_now * value)
                totals[2] += folded(value * scaled)
                totals[3] += folded(value * pre * value)

    def sum_over(stage, buffer, me, others, place, value):
        buffer[me] = value
        copies = [
            send(
                buffer.at[me],
                buffer.at[me],
                sum_send.at[stage, index],
                sum_recv.at[stage, index],
                place(other),
            )
            for index, other in enumerate(others)
        ]
        arrive(copies)
        return jnp.sum(buffer[...], axis=0)

    loads[0].wait()
    halve(0)
    pl.semaphore_wait(barrier, len(peers))
    direct = gather(0)
    halve(1)
    halve(2)
    totals[...] = jnp.zeros_like(totals)
    amps[192:256, :] = jnp.zeros((64, L), BF16)
    make_small()
    make_colat()
    arrive(direct)
    relayed = forward_on(0)
    direct = gather(1)
    make_azim(0, 8)
    arrive(relayed)
    legendre(0)
    start_z(0, 0, there, there_mid)
    arrive(direct)
    relayed = forward_on(1)
    direct = gather(2)
    make_azim(8, 16)
    arrive(relayed)
    legendre(1)
    start_z(0, 1, there, there_mid)
    arrive(direct)
    relayed = forward_on(2)
    make_azim_across(0, 16)
    pass_on(0, 0, there, there_mid, arrived)
    arrive(relayed)
    legendre(2)
    start_z(0, 2, there, there_mid)
    make_azim_across(16, 32)
    for load in loads[1:]:
        load.wait()
    wait_y(0, 0, there_mid, arrived)
    azimuth(0, lambda: pass_on(0, 1, there, there_mid, arrived))
    wait_y(0, 1, there_mid, arrived)
    azimuth(1, lambda: pass_on(0, 2, there, there_mid, arrived))
    pass_on(1, 0, home, home_mid, returned)
    wait_y(0, 2, there_mid, arrived)

    def first_back():
        wait_y(1, 0, home_mid, returned)
        legendre_back(0)
        pass_on(1, 1, home, home_mid, returned)

    azimuth(2, first_back)
    wait_y(1, 1, home_mid, returned)
    legendre_back(1)
    pass_on(1, 2, home, home_mid, returned)
    wait_x(0)
    apply(0)
    wait_y(1, 2, home_mid, returned)
    legendre_back(2)
    wait_x(1)
    apply(1)
    wait_x(2)
    apply(2)

    row = lax.broadcasted_iota(jnp.int32, (8, 128), 0)
    value = jnp.zeros((8, 128), F32)
    for index in range(4):
        value = jnp.where(row == index, jnp.sum(totals[index], axis=0, keepdims=True), value)
    value = sum_over(0, sum_y, y_me, y_others, at_y, value)
    value = sum_over(1, sum_z, z_me, z_others, at_z, value)
    value = sum_over(2, sum_x, x_me, (right, left, across), at_x, value)
    sums[...] = jnp.broadcast_to(jnp.sum(value, axis=1, keepdims=True), (8, 128))
    for copy in sent:
        copy.wait_send()


def operator(direction, residual, noise, mask, *small):
    dma = pltpu.SemaphoreType.DMA
    block = (STOKES, 8, 8, 24, 128)
    local = (FIELDS, 2, M_DEV, L_DEV)
    return pl.pallas_call(
        operator_kernel,
        in_specs=[pl.BlockSpec(memory_space=pl.ANY)] * 4 + [in_vmem()] * 5 + [in_smem()] * 2,
        out_specs=[in_vmem(), in_vmem()],
        out_shape=[jax.ShapeDtypeStruct(local, F32), jax.ShapeDtypeStruct((8, 128), F32)],
        scratch_shapes=[
            VMEM(local, F32),
            VMEM(local, F32),
            VMEM((SLOTS, STOKES, R_DEV, PHI), F32),
            VMEM((R_DEV, PHI), jnp.int32),
            VMEM((STOKES, 4, 2, COMP, M_DEV, L_DEV), BF16),
            VMEM((CYCLES, L), BF16),
            VMEM((2 * MODES, QUARTER), BF16),
            VMEM((QUARTER, 2 * MODES), BF16),
            VMEM((3, 2, 16, 128), F32),
            VMEM((2, 16, 128), jnp.int32),
            VMEM((M_DEV, 128), jnp.int32),
            VMEM((SLOTS, L), F32),
            VMEM((256, L), BF16),
            VMEM(block, BF16),
            VMEM(block, BF16),
            VMEM(block, BF16),
            VMEM((192, 2 * MODES), BF16),
            VMEM((192, QUARTER), BF16),
            VMEM(block, BF16),
            VMEM(block, BF16),
            VMEM(block, BF16),
            VMEM((256, CYCLES), BF16),
            VMEM((STOKES, 4, COMP, 2, M_DEV, L_DEV), BF16),
            VMEM((STOKES, 3, COMP, 2, M_DEV, L_DEV), BF16),
            VMEM((4, 8, 128), F32),
            VMEM((8, 8, 128), F32),
            VMEM((8, 8, 128), F32),
            VMEM((4, 8, 128), F32),
            dma((4,)),
            dma((STOKES, 4)),
            dma((STOKES, 4)),
            dma((2, STOKES, 7)),
            dma((2, STOKES, 7)),
            dma((2, STOKES, 7)),
            dma((2, STOKES, 7)),
            dma((STOKES, 3)),
            dma((STOKES, 3)),
            dma((3, 7)),
            dma((3, 7)),
        ],
        compiler_params=pltpu.CompilerParams(
            collective_id=0, has_side_effects=True, vmem_limit_bytes=60 * 1024 * 1024
        ),
        name="operator",
    )(direction, residual, noise, mask, *small)


def finish_kernel(sums, precond, solution, residual, direction, applied, out_sol, out_res, out_dir):
    norm_old, curvature, crossed, squared = (
        jnp.concatenate([sums[index : index + 1, :]] * 4, axis=1) for index in range(4)
    )
    step_size = norm_old / curvature
    norm_new = norm_old - 2.0 * step_size * crossed + step_size * step_size * squared
    ratio = norm_new / norm_old
    for field in range(COMP):
        pre = precond[pl.ds(pl.program_id(0) * COMP + field, 1), :]
        for k in range(2):
            dir_now = direction[field, k]
            res_next = residual[field, k] - step_size * applied[field, k]
            out_sol[field, k] = solution[field, k] + step_size * dir_now
            out_res[field, k] = res_next
            out_dir[field, k] = pre * res_next + ratio * dir_now


def finish(sums, precond, *arrays):
    local = (FIELDS, 2, M_DEV, L_DEV)
    field = pl.BlockSpec((COMP, 2, M_DEV, L_DEV), lambda g: (g, 0, 0, 0))
    whole = [pl.BlockSpec((8, 128), lambda g: (0, 0)), pl.BlockSpec((FIELDS, L_DEV), lambda g: (0, 0))]
    return pl.pallas_call(
        finish_kernel,
        grid=(FIELDS // COMP,),
        in_specs=whole + [field] * 4,
        out_specs=[field] * 3,
        out_shape=[jax.ShapeDtypeStruct(local, F32)] * 3,
        name="finish",
    )(sums, precond, *arrays)


def on_device(
    solution,
    residual,
    direction,
    precond,
    inv_spec,
    mixing,
    beams,
    slot_band,
    m_order,
    cycle_order,
    inv_noise,
    pix_mask,
):
    applied, sums = operator(
        direction,
        residual,
        inv_noise,
        pix_mask,
        m_order.reshape(16, 128),
        cycle_order.reshape(8, 128),
        beams,
        precond,
        inv_spec,
        mixing.T,
        slot_band,
    )
    return tuple(finish(sums, precond, solution, residual, direction, applied))


def solution(mesh):
    finer = Mesh(
        mesh.devices.reshape(mesh.shape["band"], 8, 4, 2), ("band", "blk_0", "blk_1", "blk_2")
    )
    in_specs = (
        P(None, None, BLK, "band"),
        P(None, None, BLK, "band"),
        P(None, None, BLK, "band"),
        P(None, "band"),
        P(None, "band"),
        P(),
        P(),
        P(),
        P(),
        P(),
        P("band", None, BLK, None),
        P(BLK, None),
    )
    out_specs = (P(None, None, BLK, "band"), P(None, None, BLK, "band"), P(None, None, BLK, "band"))
    return jax.shard_map(
        on_device, mesh=finer, in_specs=in_specs, out_specs=out_specs, check_vma=False
    )
```

```python
import math

import jax
import jax.numpy as jnp
from jax import lax
from jax.experimental import pallas as pl
from jax.experimental.pallas import tpu as pltpu
from jax.sharding import Mesh
from jax.sharding import PartitionSpec as P

COMP = 3
STOKES = 3
FIELDS = 9
BANDS = 9
SLOTS = 3
L = 2048
CYCLES = 1024
MODES = 2048
PHI = 4096
QUARTER = PHI // 4
M_DEV = 32
R_DEV = 16
BLOCKS = 64
L_DEV = 512
BLK = ("blk_0", "blk_1", "blk_2")
SCALE = 1.0 / math.sqrt(2048)
VMEM = pltpu.VMEM
MESH = pl.DeviceIdType.MESH
F32 = jnp.float32
BF16 = jnp.bfloat16
NT = (((1,), (1,)), ((), ()))
NN = (((1,), (0,)), ((), ()))


def in_vmem():
    return pl.BlockSpec(memory_space=VMEM)


def in_smem():
    return pl.BlockSpec(memory_space=pltpu.SMEM)


def unit_circle(turn):
    half = (((turn + 2048) & 4095) - 2048).astype(F32) * (math.pi / 4096)
    sq = half * half
    sine = half * (
        1
        + sq
        * (-1 / 6 + sq * (1 / 120 + sq * (-1 / 5040 + sq * (1 / 362880 + sq * (-1 / 39916800)))))
    )
    cosine = 1 + sq * (
        -1 / 2
        + sq
        * (
            1 / 24
            + sq * (-1 / 720 + sq * (1 / 40320 + sq * (-1 / 3628800 + sq * (1 / 479001600))))
        )
    )
    return cosine * cosine - sine * sine, 2 * sine * cosine


def first_turns(mult):
    lane = lax.broadcasted_iota(jnp.int32, mult.shape, 1)
    cosine, sine = unit_circle((mult * lane) & 4095)
    step_cos, step_sin = unit_circle((mult * 128) & 4095)
    return cosine * SCALE, sine * SCALE, step_cos, step_sin


def colat_rows(mult, store):
    cosine, sine, step_cos, step_sin = first_turns(mult)
    for tile in range(L // 128):
        store(tile, cosine.astype(BF16))
        cosine, sine = cosine * step_cos - sine * step_sin, sine * step_cos + cosine * step_sin


def azim_rows(mult, store):
    cosine, sine, step_cos, step_sin = first_turns(mult)
    for tile in range(QUARTER // 128):
        store(tile, cosine.astype(BF16), (-sine).astype(BF16))
        cosine, sine = cosine * step_cos - sine * step_sin, sine * step_cos + cosine * step_sin


STEP = 32


def azim_columns(order, first_turn, store):
    cell = lax.broadcasted_iota(jnp.int32, (STEP, 128), 0)
    cosine, sine = unit_circle((order * cell + first_turn) & 4095)
    step_cos, step_sin = unit_circle((order * STEP) & 4095)
    cosine, sine = cosine * SCALE, sine * SCALE
    for step in range(QUARTER // STEP):
        store(step, cosine.astype(BF16))
        cosine, sine = cosine * step_cos - sine * step_sin, sine * step_cos + cosine * step_sin


def spread(values, row):
    line = values[pl.ds(row, 1), :].astype(F32)
    return jnp.broadcast_to(line, (128, 128)).T.astype(jnp.int32)


def at_least(orders, first):
    l_values = first + lax.broadcasted_iota(jnp.int32, (M_DEV, 256), 1)
    return (l_values >= jnp.concatenate([orders, orders], axis=1)).astype(F32)


def partner(value, low):
    return jnp.where(low, pltpu.roll(value, 96, 1), pltpu.roll(value, 32, 1))


def folded(value):
    tiles = [
        value[8 * i : 8 * i + 8, 128 * j : 128 * j + 128]
        for i in range(value.shape[0] // 8)
        for j in range(value.shape[1] // 128)
    ]
    while len(tiles) > 1:
        tiles = [first + second for first, second in zip(tiles[::2], tiles[1::2])]
    return tiles[0]


def operator_kernel(
    direction_in,
    residual_in,
    noise_in,
    mask_in,
    m_rows,
    cycle_rows,
    beams,
    precond,
    inv_spec,
    mixing,
    slot_band,
    applied,
    sums,
    direction,
    residual,
    noise,
    mask,
    gathered,
    colat,
    azim,
    azim_across,
    turns,
    order_lanes,
    orders,
    beam,
    amps,
    there,
    there_mid,
    arrived,
    turned,
    weighted,
    home,
    home_mid,
    returned,
    flipped,
    combined,
    parts,
    totals,
    sum_y,
    sum_z,
    sum_x,
    load_sem,
    gather_send,
    gather_recv,
    z_send,
    z_recv,
    y_send,
    y_recv,
    x_send,
    x_recv,
    sum_send,
    sum_recv,
):
    x_me = lax.axis_index("band")
    z_me = lax.axis_index("blk_0")
    y_me = lax.axis_index("blk_1") * 2 + lax.axis_index("blk_2")
    right, left, across = (lax.rem(x_me + off, 4) for off in (1, 3, 2))
    z_others = [lax.rem(z_me + off, 8) for off in range(1, 8)]
    y_others = [lax.rem(y_me + off, 8) for off in range(1, 8)]

    def at_x(index):
        return {"band": index}

    def at_z(index):
        return {"blk_0": index}

    def at_y(index):
        return {"blk_1": lax.div(index, 2), "blk_2": lax.rem(index, 2)}

    peers = [at_x(i) for i in (right, left, across)]
    peers += [at_z(i) for i in z_others] + [at_y(i) for i in y_others]
    barrier = pltpu.get_barrier_semaphore()
    for peer in peers:
        pl.semaphore_signal(barrier, inc=1, device_id=peer, device_id_type=MESH)

    loads = [
        pltpu.make_async_copy(source, target, load_sem.at[index])
        for index, (source, target) in enumerate(
            ((direction_in, direction), (mask_in, mask), (noise_in, noise), (residual_in, residual))
        )
    ]
    for load in loads:
        load.start()

    sent = []

    def describe(source, target, send_sem, recv_sem, peer):
        return pltpu.make_async_remote_copy(
            src_ref=source,
            dst_ref=target,
            send_sem=send_sem,
            recv_sem=recv_sem,
            device_id=peer,
            device_id_type=MESH,
        )

    def send(*ends):
        copy = describe(*ends)
        copy.start()
        sent.append(copy)
        return copy

    def arrive(copies):
        for copy in copies:
            copy.wait_recv()

    def halve(s):
        for k in range(2):
            for c in range(COMP):
                gathered[s, x_me, k, c] = direction[c * 3 + s, k].astype(BF16)

    def gather(s):
        return [
            send(
                gathered.at[s, x_me],
                gathered.at[s, x_me],
                gather_send.at[s, way],
                gather_recv.at[s, way],
                at_x(peer),
            )
            for way, peer in enumerate((right, left))
        ]

    def forward_on(s):
        return [
            send(
                gathered.at[s, source, way],
                gathered.at[s, source, way],
                gather_send.at[s, 2 + way],
                gather_recv.at[s, 2 + way],
                at_x(peer),
            )
            for way, (source, peer) in enumerate(((left, right), (right, left)))
        ]

    def make_colat():
        @pl.loop(0, CYCLES // 128)
        def _(block):
            mult = 2 * spread(cycle_rows, block) + 1
            for sub in range(4):
                rows = pl.ds(pl.multiple_of(block * 128 + sub * 32, 32), 32)

                def put(tile, value):
                    colat[rows, tile * 128 : (tile + 1) * 128] = value

                colat_rows(mult[sub * 32 : sub * 32 + 32], put)

    def make_azim(begin, end):
        @pl.loop(begin, end)
        def _(block):
            mult = spread(m_rows, block)
            for sub in range(4):
                first = block * 256 + sub * 64
                real_rows = pl.ds(pl.multiple_of(first, 32), 32)
                imag_rows = pl.ds(pl.multiple_of(first + 32, 32), 32)

                def put(tile, real, imag):
                    azim[real_rows, tile * 128 : (tile + 1) * 128] = real
                    azim[imag_rows, tile * 128 : (tile + 1) * 128] = imag

                azim_rows(mult[sub * 32 : sub * 32 + 32], put)

    def make_azim_across(begin, end):
        @pl.loop(begin, end)
        def _(tile):
            cols = pl.ds(pl.multiple_of(tile * 128, 128), 128)
            order = order_lanes[tile % 2, pl.ds(tile // 2, 1), :]
            part = lax.broadcasted_iota(jnp.int32, (1, 128), 1) & 32

            def put(step, value):
                azim_across[step * STEP : (step + 1) * STEP, cols] = value

            azim_columns(order, part * 32, put)

    mix = [[None] * COMP for _ in range(SLOTS)]
    for x in range(SLOTS):
        slot = slot_band[x_me * SLOTS + x]
        for c in range(COMP):
            mix[x][c] = jnp.where(slot < BANDS, mixing[c, jnp.minimum(slot, BANDS - 1)], 0.0)

    def make_small():
        place = lax.broadcasted_iota(jnp.int32, (16, 128), 1)
        line = m_rows[...]
        even = jnp.where(
            place < 32, line, jnp.where(place < 96, pltpu.roll(line, 32, 1), pltpu.roll(line, 64, 1))
        )
        odd = jnp.where(
            place < 32, pltpu.roll(line, 64, 1), jnp.where(place < 96, pltpu.roll(line, 96, 1), line)
        )
        way = jnp.where((place & 63) < 32, 1.0, -1.0)
        for parity, value in enumerate((even, odd)):
            order_lanes[parity] = value
            phase = value & 3
            turns[0, parity] = jnp.where((value & 1) == 0, 1.0, -1.0)
            turns[1, parity] = jnp.where(phase == 0, 1.0, jnp.where(phase == 2, -1.0, 0.0))
            turns[2, parity] = way * jnp.where(
                phase == 1, 1.0, jnp.where(phase == 3, -1.0, 0.0)
            )
        for x in range(SLOTS):
            slot = slot_band[x_me * SLOTS + x]
            total = jnp.zeros((1, L), F32)
            for band in range(BANDS):
                total = jnp.where(slot == band, beams[band : band + 1, :], total)
            beam[x : x + 1, :] = total
        blk = z_me * 8 + y_me
        all_orders = spread(m_rows, lax.div(blk, 4))
        for sub in range(4):

            @pl.when(lax.rem(blk, 4) == sub)
            def _():
                orders[...] = all_orders[sub * 32 : sub * 32 + 32]

    def turns_of(tile):
        return [turns[index, tile % 2, pl.ds(tile // 2, 1), :] for index in range(3)]

    lane = lax.broadcasted_iota(jnp.int32, (R_DEV, 128), 1)
    on_left = lane < 64
    on_left8 = on_left[:8]
    low = (lane & 63) < 32

    def legendre(s):
        @pl.loop(0, L // 256, unroll=2)
        def _(block):
            first = pl.multiple_of(block * 256, 256)
            piece = block // 2
            inner = pl.ds(pl.multiple_of((block % 2) * 256, 256), 256)
            triangle = at_least(orders[...], first)
            for k in range(2):
                comps = [gathered[s, piece, k, c, :, inner].astype(F32) for c in range(COMP)]
                for x in range(SLOTS):
                    mixed = mix[x][0] * comps[0]
                    for c in range(1, COMP):
                        mixed = mixed + mix[x][c] * comps[c]
                    row = (x * 2 + k) * M_DEV
                    value = mixed * beam[x : x + 1, pl.ds(first, 256)] * triangle
                    amps[row : row + M_DEV, pl.ds(first, 256)] = value.astype(BF16)

        @pl.loop(0, CYCLES // 256, unroll=2)
        def _(block):
            rows = pl.ds(pl.multiple_of(block * 256, 256), 256)
            side = lax.dot_general(colat[rows, :], amps[...], NT, preferred_element_type=F32)
            main = side[:, :128].reshape(2, 8, 16, 128)
            tail = side[:, 128:].reshape(16, 16, 128)
            wide = lax.broadcasted_iota(jnp.int32, (128, 128), 1) < 64
            packed = jnp.where(
                wide,
                tail[:, :8].reshape(128, 128),
                pltpu.roll(tail[:, 8:].reshape(128, 128), 64, 1),
            )
            there[s, pl.ds(block * 2, 2), :, 0:16, :] = main.astype(BF16)
            there[s, pl.ds(block * 2, 2), :, 16:24, :] = packed.reshape(2, 8, 8, 128).astype(BF16)

    def z_copy(way, s, off, source, middle):
        other = lax.rem(z_me + off, 8)
        return describe(
            source.at[s, other],
            middle.at[s, z_me],
            z_send.at[way, s, off - 1],
            z_recv.at[way, s, off - 1],
            at_z(other),
        )

    def start_z(way, s, source, middle):
        for off in (1, 7, 2, 6, 3, 5, 4):
            z_copy(way, s, off, source, middle).start()

    def y_copy(way, s, index, source, target):
        return describe(
            source, target, y_send.at[way, s, index], y_recv.at[way, s, index], at_y(y_others[index])
        )

    def pass_on(way, s, source, middle, target):
        for off in (0, 1, 7, 2, 6, 3, 5, 4):
            plane = lax.rem(z_me + 8 - off, 8)
            held = source if off == 0 else middle
            if off:
                copy = z_copy(way, s, off, source, middle)
                copy.wait_recv()
                sent.append(copy)
            for index, other in enumerate(y_others):
                y_copy(
                    way, s, index, held.at[s, plane, other], target.at[s, plane, y_me]
                ).start()
            target[s, plane, y_me] = held[s, plane, y_me]

    def wait_y(way, s, middle, target):
        for index, other in enumerate(y_others):
            copy = y_copy(way, s, index, middle.at[s, :, other], target.at[s, :, y_me])
            copy.wait_recv()
            sent.append(copy)

    def azimuth(s, between):
        @pl.loop(0, BLOCKS // 2, unroll=4)
        def _(tile):
            cols = pl.ds(pl.multiple_of(tile * 128, 128), 128)
            sign, cosine, sine = turns_of(tile)
            plane, place = tile // 4, (tile % 4) * 2
            first = arrived[s, plane, place, 0:16, :].astype(F32)
            second = arrived[s, plane, place + 1, 0:16, :].astype(F32)
            third = arrived[s, plane, place, 16:24, :].astype(F32)
            fourth = arrived[s, plane, place + 1, 16:24, :].astype(F32)
            values = [
                jnp.where(on_left, first, pltpu.roll(second, 64, 1)),
                jnp.where(on_left, pltpu.roll(first, 64, 1), second),
                jnp.concatenate(
                    [
                        jnp.where(on_left8, third, pltpu.roll(fourth, 64, 1)),
                        jnp.where(on_left8, pltpu.roll(third, 64, 1), fourth),
                    ],
                    axis=0,
                ),
            ]
            for x, value in enumerate(values):
                straight = cosine * value
                crossed = sine * partner(value, low)
                for q, part in enumerate(
                    (value, straight - crossed, sign * value, straight + crossed)
                ):
                    row = q * 48 + x * R_DEV
                    turned[row : row + R_DEV, cols] = part.astype(BF16)

        @pl.loop(0, QUARTER // 256, unroll=2)
        def _(block):
            start = pl.multiple_of(block * 256, 256)
            cols = pl.ds(start, 256)
            sky = lax.dot_general(turned[...], azim[:, cols], NN, preferred_element_type=F32)
            for q in range(4):
                cells = pl.ds(pl.multiple_of(q * QUARTER + start, 256), 256)
                keep = mask[:, cells].astype(F32)
                for x in range(SLOTS):
                    row = q * 48 + x * R_DEV
                    weight = noise[x, s, :, cells] * keep
                    weighted[row : row + R_DEV, cols] = (
                        weight * sky[row : row + R_DEV, :]
                    ).astype(BF16)

        between()

        @pl.loop(1, 9)
        def _(off):
            home_plane = lax.rem(z_me + off, 8)
            backs = []
            for half in range(2):
                cols = pl.ds(pl.multiple_of(home_plane * 512 + half * 256, 256), 256)
                backs.append(
                    lax.dot_general(
                        weighted[...], azim_across[:, cols], NN, preferred_element_type=F32
                    )
                )
            for inner in range(4):
                tile = home_plane * 4 + inner
                back, sub = backs[inner // 2], inner % 2
                sign, cosine, sine = turns_of(tile)
                lanes = slice(sub * 128, sub * 128 + 128)
                values = []
                for x in range(SLOTS):
                    b0, b1, b2, b3 = (
                        back[q * 48 + x * R_DEV : q * 48 + x * R_DEV + R_DEV, lanes]
                        for q in range(4)
                    )
                    values.append(
                        b0 + sign * b2 + cosine * (b1 + b3) + sine * partner(b1 - b3, low)
                    )
                zero, one, two = values
                plane, place = home_plane, inner * 2
                home[s, plane, place, 0:16, :] = jnp.where(
                    on_left, zero, pltpu.roll(one, 64, 1)
                ).astype(BF16)
                home[s, plane, place + 1, 0:16, :] = jnp.where(
                    on_left, pltpu.roll(zero, 64, 1), one
                ).astype(BF16)
                home[s, plane, place, 16:24, :] = jnp.where(
                    on_left8, two[:8], pltpu.roll(two[8:], 64, 1)
                ).astype(BF16)
                home[s, plane, place + 1, 16:24, :] = jnp.where(
                    on_left8, pltpu.roll(two[:8], 64, 1), two[8:]
                ).astype(BF16)

            @pl.when(off < 8)
            def _():
                z_copy(1, s, off, home, home_mid).start()

    def legendre_back(s):
        @pl.loop(0, 8, unroll=4)
        def _(plane):
            cols = pl.ds(pl.multiple_of(plane * 128, 128), 128)
            main = returned[s, plane, :, 0:16, :].astype(F32).reshape(128, 128)
            tail = returned[s, plane, :, 16:24, :].astype(F32)
            swapped = pltpu.roll(tail.reshape(64, 128), 64, 1).reshape(8, 8, 128)
            both = jnp.concatenate([tail, swapped], axis=1).reshape(128, 128)
            flipped[0:128, cols] = main.T.astype(BF16)
            flipped[128:256, cols] = both.T.astype(BF16)

        @pl.loop(1, 5)
        def _(off):
            piece = lax.rem(x_me + off, 4)
            for half in range(2):
                start = pl.multiple_of(piece * L_DEV + half * 256, 256)
                harm = lax.dot_general(
                    flipped[0:192, :],
                    colat[:, pl.ds(start, 256)],
                    NN,
                    preferred_element_type=F32,
                )
                triangle = at_least(orders[...], start)
                inner = slice(half * 256, half * 256 + 256)
                for k in range(2):
                    shaped = []
                    for x in range(SLOTS):
                        row = (x * 2 + k) * M_DEV
                        shaped.append(
                            harm[row : row + M_DEV, :]
                            * beam[x : x + 1, pl.ds(start, 256)]
                            * triangle
                        )
                    for c in range(COMP):
                        total = mix[0][c] * shaped[0]
                        for x in range(1, SLOTS):
                            total = total + mix[x][c] * shaped[x]
                        combined[s, piece, c, k, :, inner] = total.astype(BF16)

            @pl.when(off < 4)
            def _():
                x_copy(s, off).start()

    def x_copy(s, off):
        other = lax.rem(x_me + off, 4)
        return describe(
            combined.at[s, other],
            parts.at[s, off - 1],
            x_send.at[s, off - 1],
            x_recv.at[s, off - 1],
            at_x(other),
        )

    def wait_x(s):
        for off in range(1, 4):
            copy = x_copy(s, off)
            copy.wait_recv()
            sent.append(copy)

    def apply(s):
        for c in range(COMP):
            field = c * 3 + s
            pre = precond[field : field + 1, :]
            prior = inv_spec[field : field + 1, :]
            for k in range(2):
                total = combined[s, x_me, c, k].astype(F32)
                for index in range(3):
                    total = total + parts[s, index, c, k].astype(F32)
                dir_now = direction[field, k]
                res_now = residual[field, k]
                value = prior * dir_now + total
                applied[field, k] = value
                scaled = pre * res_now
                totals[0] += folded(res_now * scaled)
                totals[1] += folded(dir_now * value)
                totals[2] += folded(value * scaled)
                totals[3] += folded(value * pre * value)

    def sum_over(stage, buffer, me, others, place, value):
        buffer[me] = value
        copies = [
            send(
                buffer.at[me],
                buffer.at[me],
                sum_send.at[stage, index],
                sum_recv.at[stage, index],
                place(other),
            )
            for index, other in enumerate(others)
        ]
        arrive(copies)
        return jnp.sum(buffer[...], axis=0)

    loads[0].wait()
    halve(0)
    pl.semaphore_wait(barrier, len(peers))
    direct = gather(0)
    halve(1)
    halve(2)
    totals[...] = jnp.zeros_like(totals)
    amps[192:256, :] = jnp.zeros((64, L), BF16)
    make_small()
    make_colat()
    arrive(direct)
    relayed = forward_on(0)
    direct = gather(1)
    make_azim(0, 8)
    arrive(relayed)
    legendre(0)
    start_z(0, 0, there, there_mid)
    arrive(direct)
    relayed = forward_on(1)
    direct = gather(2)
    make_azim(8, 16)
    arrive(relayed)
    legendre(1)
    start_z(0, 1, there, there_mid)
    arrive(direct)
    relayed = forward_on(2)
    make_azim_across(0, 16)
    pass_on(0, 0, there, there_mid, arrived)
    arrive(relayed)
    legendre(2)
    start_z(0, 2, there, there_mid)
    make_azim_across(16, 32)
    for load in loads[1:]:
        load.wait()
    wait_y(0, 0, there_mid, arrived)
    azimuth(0, lambda: pass_on(0, 1, there, there_mid, arrived))
    wait_y(0, 1, there_mid, arrived)
    azimuth(1, lambda: pass_on(0, 2, there, there_mid, arrived))
    pass_on(1, 0, home, home_mid, returned)
    wait_y(0, 2, there_mid, arrived)

    def first_back():
        wait_y(1, 0, home_mid, returned)
        legendre_back(0)
        pass_on(1, 1, home, home_mid, returned)

    azimuth(2, first_back)
    wait_y(1, 1, home_mid, returned)
    legendre_back(1)
    pass_on(1, 2, home, home_mid, returned)
    wait_x(0)
    apply(0)
    wait_y(1, 2, home_mid, returned)
    legendre_back(2)
    wait_x(1)
    apply(1)
    wait_x(2)
    apply(2)

    row = lax.broadcasted_iota(jnp.int32, (8, 128), 0)
    value = jnp.zeros((8, 128), F32)
    for index in range(4):
        value = jnp.where(row == index, jnp.sum(totals[index], axis=0, keepdims=True), value)
    value = sum_over(0, sum_y, y_me, y_others, at_y, value)
    value = sum_over(1, sum_z, z_me, z_others, at_z, value)
    value = sum_over(2, sum_x, x_me, (right, left, across), at_x, value)
    sums[...] = jnp.broadcast_to(jnp.sum(value, axis=1, keepdims=True), (8, 128))
    for copy in sent:
        copy.wait_send()


def operator(direction, residual, noise, mask, *small):
    dma = pltpu.SemaphoreType.DMA
    block = (STOKES, 8, 8, 24, 128)
    local = (FIELDS, 2, M_DEV, L_DEV)
    return pl.pallas_call(
        operator_kernel,
        in_specs=[pl.BlockSpec(memory_space=pl.ANY)] * 4 + [in_vmem()] * 5 + [in_smem()] * 2,
        out_specs=[in_vmem(), in_vmem()],
        out_shape=[jax.ShapeDtypeStruct(local, F32), jax.ShapeDtypeStruct((8, 128), F32)],
        scratch_shapes=[
            VMEM(local, F32),
            VMEM(local, F32),
            VMEM((SLOTS, STOKES, R_DEV, PHI), F32),
            VMEM((R_DEV, PHI), jnp.int32),
            VMEM((STOKES, 4, 2, COMP, M_DEV, L_DEV), BF16),
            VMEM((CYCLES, L), BF16),
            VMEM((2 * MODES, QUARTER), BF16),
            VMEM((QUARTER, 2 * MODES), BF16),
            VMEM((3, 2, 16, 128), F32),
            VMEM((2, 16, 128), jnp.int32),
            VMEM((M_DEV, 128), jnp.int32),
            VMEM((SLOTS, L), F32),
            VMEM((256, L), BF16),
            VMEM(block, BF16),
            VMEM(block, BF16),
            VMEM(block, BF16),
            VMEM((192, 2 * MODES), BF16),
            VMEM((192, QUARTER), BF16),
            VMEM(block, BF16),
            VMEM(block, BF16),
            VMEM(block, BF16),
            VMEM((256, CYCLES), BF16),
            VMEM((STOKES, 4, COMP, 2, M_DEV, L_DEV), BF16),
            VMEM((STOKES, 3, COMP, 2, M_DEV, L_DEV), BF16),
            VMEM((4, 8, 128), F32),
            VMEM((8, 8, 128), F32),
            VMEM((8, 8, 128), F32),
            VMEM((4, 8, 128), F32),
            dma((4,)),
            dma((STOKES, 4)),
            dma((STOKES, 4)),
            dma((2, STOKES, 7)),
            dma((2, STOKES, 7)),
            dma((2, STOKES, 7)),
            dma((2, STOKES, 7)),
            dma((STOKES, 3)),
            dma((STOKES, 3)),
            dma((3, 7)),
            dma((3, 7)),
        ],
        compiler_params=pltpu.CompilerParams(
            collective_id=0, has_side_effects=True, vmem_limit_bytes=60 * 1024 * 1024
        ),
        name="operator",
    )(direction, residual, noise, mask, *small)


def finish_kernel(sums, precond, solution, residual, direction, applied, out_sol, out_res, out_dir):
    norm_old, curvature, crossed, squared = (
        jnp.concatenate([sums[index : index + 1, :]] * 4, axis=1) for index in range(4)
    )
    step_size = norm_old / curvature
    norm_new = norm_old - 2.0 * step_size * crossed + step_size * step_size * squared
    ratio = norm_new / norm_old
    for field in range(COMP):
        pre = precond[pl.ds(pl.program_id(0) * COMP + field, 1), :]
        for k in range(2):
            dir_now = direction[field, k]
            res_next = residual[field, k] - step_size * applied[field, k]
            out_sol[field, k] = solution[field, k] + step_size * dir_now
            out_res[field, k] = res_next
            out_dir[field, k] = pre * res_next + ratio * dir_now


def finish(sums, precond, *arrays):
    local = (FIELDS, 2, M_DEV, L_DEV)
    field = pl.BlockSpec((COMP, 2, M_DEV, L_DEV), lambda g: (g, 0, 0, 0))
    whole = [pl.BlockSpec((8, 128), lambda g: (0, 0)), pl.BlockSpec((FIELDS, L_DEV), lambda g: (0, 0))]
    return pl.pallas_call(
        finish_kernel,
        grid=(FIELDS // COMP,),
        in_specs=whole + [field] * 4,
        out_specs=[field] * 3,
        out_shape=[jax.ShapeDtypeStruct(local, F32)] * 3,
        name="finish",
    )(sums, precond, *arrays)


def on_device(
    solution,
    residual,
    direction,
    precond,
    inv_spec,
    mixing,
    beams,
    slot_band,
    m_order,
    cycle_order,
    inv_noise,
    pix_mask,
):
    applied, sums = operator(
        direction,
        residual,
        inv_noise,
        pix_mask,
        m_order.reshape(16, 128),
        cycle_order.reshape(8, 128),
        beams,
        precond,
        inv_spec,
        mixing.T,
        slot_band,
    )
    return tuple(finish(sums, precond, solution, residual, direction, applied))


def solution(mesh):
    finer = Mesh(
        mesh.devices.reshape(mesh.shape["band"], 8, 4, 2), ("band", "blk_0", "blk_1", "blk_2")
    )
    in_specs = (
        P(None, None, BLK, "band"),
        P(None, None, BLK, "band"),
        P(None, None, BLK, "band"),
        P(None, "band"),
        P(None, "band"),
        P(),
        P(),
        P(),
        P(),
        P(),
        P("band", None, BLK, None),
        P(BLK, None),
    )
    out_specs = (P(None, None, BLK, "band"), P(None, None, BLK, "band"), P(None, None, BLK, "band"))
    return jax.shard_map(
        on_device, mesh=finer, in_specs=in_specs, out_specs=out_specs, check_vma=False
    )
```
